8 devices in a mesh: dp: 1 (over z), sp: 8 (over x, y, core).
Axes of the slice: x: 2, y: 2, z: 1, core: 2. Of those that a mesh axis runs over, the one named last changes fastest.
Arguments:
- x: bfloat16 [1024, 5120], P(('dp', 'sp'))
- gain: bfloat16 [5120], replicated
- wq: bfloat16 [5120, 4096], replicated
- wk: bfloat16 [5120, 1024], replicated
- wv: bfloat16 [5120, 1024], replicated
- wo: bfloat16 [4096, 5120], replicated
Outputs:
- output: bfloat16 [1024, 5120], P(('dp', 'sp'))
All inputs are finite; a program needn't handle non-finite values.
Results may differ from the reference program's by a relative error of at most 0.012.
Values are sent between devices in bfloat16 or wider.
A program may use at most 2 GiB of HBM per device.

```python
import jax
import jax.numpy as jnp
from jax import lax

ROWS = 1024
D = 5120
HEADS = 32
KV_HEADS = 8
HEAD = 128
THETA = 10000


def setup_inputs(seed: int = 0, part: int = 0) -> dict:
    kx, kn, kq, kk, kv, ko = jax.random.split(jax.random.key(seed), 6)

    def weights(key, rows, columns):
        return jax.random.normal(key, (rows, columns), jnp.float32) * rows**-0.5

    drawn = {
        "x": jax.random.normal(jax.random.fold_in(kx, part), (ROWS, D), jnp.float32),
        "gain": 1 + 0.1 * jax.random.normal(kn, (D,), jnp.float32),
        "wq": 2 * weights(kq, D, HEADS * HEAD),
        "wk": 2 * weights(kk, D, KV_HEADS * HEAD),
        "wv": 4 * weights(kv, D, KV_HEADS * HEAD),
        "wo": weights(ko, HEADS * HEAD, D),
    }
    return {k: v.astype(jnp.bfloat16) for k, v in drawn.items()}


def normed(x, gain):
    wide = x.astype(jnp.float32)
    scale = lax.rsqrt(jnp.mean(wide * wide, -1, keepdims=True) + 1e-6)
    return (wide * scale * gain.astype(jnp.float32)).astype(jnp.bfloat16)


def turned(t, place, theta):
    half = t.shape[-1] // 2
    angle = place.astype(jnp.float32)[:, None] * theta ** (-jnp.arange(half, dtype=jnp.float32) / half)
    cos, sin = jnp.cos(angle)[:, None], jnp.sin(angle)[:, None]
    a, b = t[..., :half].astype(jnp.float32), t[..., half:].astype(jnp.float32)
    return jnp.concatenate([a * cos - b * sin, b * cos + a * sin], -1).astype(jnp.bfloat16)


def matmul(a, w):
    return jnp.dot(a, w, preferred_element_type=jnp.float32).astype(jnp.bfloat16)


def einsum(form, a, b):
    return jnp.einsum(form, a.astype(jnp.float32), b.astype(jnp.float32))


def attention(q, k, v):
    scores = einsum("tgsd,ugd->gstu", q, k) * q.shape[-1] ** -0.5
    token = jnp.arange(q.shape[0])
    scores = jnp.where(token[:, None] >= token, scores, -jnp.inf)
    weights = jax.nn.softmax(scores, -1).astype(jnp.bfloat16)
    return einsum("gstu,ugd->tgsd", weights, v).astype(jnp.bfloat16)


def reference(x, gain, wq, wk, wv, wo):
    a, place = normed(x, gain), jnp.arange(ROWS)
    q = turned(matmul(a, wq).reshape(ROWS, HEADS, HEAD), place, THETA).reshape(ROWS, KV_HEADS, -1, HEAD)
    k = turned(matmul(a, wk).reshape(ROWS, KV_HEADS, HEAD), place, THETA)
    v = matmul(a, wv).reshape(ROWS, KV_HEADS, HEAD)
    seen = attention(q, k, v).reshape(ROWS, HEADS * HEAD)
    return (x.astype(jnp.float32) + jnp.dot(seen, wo, preferred_element_type=jnp.float32)).astype(jnp.bfloat16)
```

```python
import functools

import jax
import jax.numpy as jnp
import numpy as np
from jax import lax
from jax.experimental import pallas as pl
from jax.experimental.pallas import tpu as pltpu
from jax.sharding import PartitionSpec as P

HEAD = 128
THETA = 10000
LOG2E = 1.4426950408889634
HIDDEN = -2e30
E = HEAD**-0.5 * LOG2E
F32, BF16 = jnp.float32, jnp.bfloat16

OWN = 128
TOK = 256
D = 5120
N = 512
COLS = D // 2
NB = COLS // N
SLOTS = 8


def tables(rows):
    half = HEAD // 2
    power = np.float32(THETA) ** (-np.arange(half, dtype=np.float32) / np.float32(half))
    angle = np.arange(rows, dtype=np.float32)[:, None] * power.astype(np.float32)
    cos, sin = np.cos(angle.astype(np.float32)), np.sin(angle.astype(np.float32))
    return np.concatenate([cos, cos], 1).astype(np.float32), np.concatenate([-sin, sin], 1).astype(np.float32)


def _dot(a, b, ca=1, cb=0):
    return lax.dot_general(a, b, (((ca,), (cb,)), ((), ())), preferred_element_type=F32)


def kernel(x_hbm, gain_hbm, wq, wk, wv, wo, cos_hbm, sin_hbm, y_hbm,
           W, xr, a, gain, cos, sin, q, kv, acc, top_s, mine, theirs, y, yo,
           wsem, xsem, xsend, xrecv, tsem, ksend, krecv, rsend, asend, arecv, ysend, yrecv, ysem):
    me = lax.axis_index("sp")
    chip, c = me // 2, me % 2
    partner = chip * 2 + (1 - c)

    def there(chip_to):
        return {"sp": chip_to * 2 + c}

    def load_kv(pair):
        for i in range(2):
            at = pl.multiple_of((4 * c + 2 * pair + i) * HEAD, HEAD)
            pltpu.make_async_copy(wk.at[:, pl.ds(at, HEAD)], W.at[pair, :, pl.ds(i * 256, HEAD)], wsem.at[pair]).start()
            pltpu.make_async_copy(wv.at[:, pl.ds(at, HEAD)], W.at[pair, :, pl.ds(i * 256 + HEAD, HEAD)], wsem.at[pair]).start()

    def load_q(s):
        at = pl.multiple_of(2048 * c + N * s, N)
        pltpu.make_async_copy(wq.at[:, pl.ds(at, N)], W.at[2 + s], wsem.at[2 + s]).start()

    def load_o(k, slot):
        side = c if k % 2 == 0 else 1 - c
        row = pl.multiple_of(2048 * side + 1024 * (k // 2), 1024)
        for n in range(NB):
            at = pl.multiple_of(COLS * c + N * n, N)
            pltpu.make_async_copy(wo.at[pl.ds(row, 1024), pl.ds(at, N)], W.at[slot, pl.ds(1024 * n, 1024), :], wsem.at[slot]).start()

    def wait_slot(s):
        pltpu.make_async_copy(W.at[s], W.at[s], wsem.at[s]).wait()

    own_rows = pl.ds(pl.multiple_of(c * OWN, OWN), OWN)
    their_rows = pl.ds(pl.multiple_of((1 - c) * OWN, OWN), OWN)
    x_in = pltpu.make_async_copy(x_hbm, xr.at[own_rows], xsem)
    x_in.start()
    places = pl.ds(pl.multiple_of(chip * TOK, TOK), TOK)
    small = [pltpu.make_async_copy(gain_hbm, gain, tsem.at[0]),
             pltpu.make_async_copy(cos_hbm.at[places], cos, tsem.at[1]),
             pltpu.make_async_copy(sin_hbm.at[places], sin, tsem.at[2])]
    for s in small:
        s.start()
    load_kv(0)
    load_kv(1)

    barrier = pltpu.get_barrier_semaphore()
    for peer in (partner, (chip + 1 - 2 * (chip % 2)) * 2 + c, (chip + 2) % 4 * 2 + c):
        pl.semaphore_signal(barrier, inc=1, device_id={"sp": peer}, device_id_type=pl.DeviceIdType.MESH)
    pl.semaphore_wait(barrier, 3)

    x_out = pltpu.make_async_remote_copy(x_hbm, xr.at[own_rows], xsend, xrecv, {"sp": partner}, pl.DeviceIdType.MESH)
    x_out.start()
    load_q(0)
    small[0].wait()
    x_in.wait()

    def norm(first):
        g = gain[...].astype(F32)

        def body(i, _):
            rows = pl.ds(pl.multiple_of(first + i * 16, 16), 16)
            wide = xr[rows, :].astype(F32)
            scale = lax.rsqrt(jnp.mean(wide * wide, -1, keepdims=True) + 1e-6)
            a[rows, :] = (wide * scale * g).astype(BF16)

        lax.fori_loop(0, OWN // 16, body, None)

    def turn(t, rows):
        t = t.astype(BF16).astype(F32)
        return (t * cos[rows, :] + pltpu.roll(t, 64, 1) * sin[rows, :]).astype(BF16)

    def unit_copy(j, pair, half, sem, chip_to):
        return pltpu.make_async_remote_copy(kv.at[j, pair, half], kv.at[j, pair, half], sem, krecv.at[j, pair, half],
                                            there(chip_to), pl.DeviceIdType.MESH)

    def make_kv(half, pair):
        rows = pl.ds(pl.multiple_of(half * OWN, OWN), OWN)
        r = _dot(a[rows, :], W[pair])
        for i in range(2):
            kv[chip, pair, half, i, :, :HEAD] = turn(r[:, i * 256 : i * 256 + HEAD], rows)
            kv[chip, pair, half, i, :, HEAD:] = r[:, i * 256 + HEAD : (i + 1) * 256].astype(BF16)

        @pl.when(chip != 3)
        def _():
            unit_copy(chip, pair, half, ksend.at[0, pair, half], jnp.where(chip == 0, 1, 3)).start()

        @pl.when(chip == 0)
        def _():
            unit_copy(chip, pair, half, ksend.at[1, pair, half], 2).start()

    norm(c * OWN)
    small[1].wait()
    small[2].wait()
    for pair in range(2):
        wait_slot(pair)
        make_kv(c, pair)
        load_q(1 + pair)
    x_out.wait_recv()
    norm((1 - c) * OWN)
    for pair in range(2):
        make_kv(1 - c, pair)
    load_q(3)
    load_o(0, 6)

    for s in range(4):
        wait_slot(2 + s)
        r = _dot(a[...], W[2 + s])
        for g in range(4):
            q[s, g * TOK : (g + 1) * TOK, :] = turn(r[:, g * HEAD : (g + 1) * HEAD], pl.ds(0, TOK))
        if s < 3:
            load_o(1 + s, (7, 0, 1)[s])

    def relay(pair):
        for p in (1, 2):
            @pl.when(chip == p)
            def _():
                move = unit_copy(0, pair, p - 1, rsend.at[pair, p - 1], 3)
                move.wait_recv()
                move.start()

    relay(0)

    def attend(j, pair, first):
        mask = None
        if first:
            mask = lax.broadcasted_iota(jnp.int32, (TOK, TOK), 0) <= lax.broadcasted_iota(jnp.int32, (TOK, TOK), 1)
        for i in range(2):
            h = 2 * pair + i
            keys = jnp.concatenate([kv[j, pair, t, i, :, :HEAD] for t in range(2)], 0)
            values = jnp.concatenate([kv[j, pair, t, i, :, HEAD:] for t in range(2)], 0)
            vt = jnp.concatenate([values.T, jnp.ones((8, TOK), BF16)], 0)
            scores = [_dot(keys, q[h, g * TOK : (g + 1) * TOK, :], 1, 1) for g in range(4)]
            for g, s in enumerate(scores):
                at = slice(g * TOK, (g + 1) * TOK)
                if first:
                    s = jnp.where(mask, s, HIDDEN)
                    top = s.max(axis=0, keepdims=True)
                    p = jnp.exp2((s - top) * E).astype(BF16)
                    acc[h, :, at] = _dot(vt, p)
                else:
                    old = top_s[h, :, at]
                    top = jnp.maximum(old, s.max(axis=0, keepdims=True))
                    p = jnp.exp2((s - top) * E).astype(BF16)
                    acc[h, :, at] = acc[h, :, at] * jnp.exp2((old - top) * E) + _dot(vt, p)
                top_s[h, :, at] = top

    def wait_units(j, pair):
        for half in range(2):
            @pl.when(jnp.logical_not((j == 0) & (chip == half + 1)))
            def _():
                unit_copy(j, pair, half, ksend.at[0, pair, half], chip).wait_recv()

    lax.fori_loop(0, 2, lambda pair, _: attend(chip, pair, True), None)
    relay(1)

    def early(t, _):
        s, pair = t // 2, t % 2
        j = jnp.where(chip == 3, 1 + s, 0)
        wait_units(j, pair)

        @pl.when((chip == 3) & (j == 1))
        def _():
            for half in range(2):
                unit_copy(1, pair, half, rsend.at[pair, half], 2).start()

        attend(j, pair, False)

    lax.fori_loop(0, 2 * jnp.maximum(chip - 1, 0), early, None)

    def swap(pair):
        return pltpu.make_async_remote_copy(mine.at[pair], theirs.at[pair], asend.at[pair], arecv.at[pair], {"sp": partner},
                                            pl.DeviceIdType.MESH)

    def late(pair, _):
        @pl.when(chip > 0)
        def _():
            j = jnp.where(chip == 2, 1, 0)
            wait_units(j, pair)
            attend(j, pair, False)

        for i in range(2):
            h = 2 * pair + i
            for g in range(4):
                at = slice(g * TOK, (g + 1) * TOK)
                out = acc[h, :HEAD, at] * (1 / acc[h, HEAD : HEAD + 1, at])
                mine[pair, :, (4 * i + g) * HEAD : (4 * i + g + 1) * HEAD] = out.T.astype(BF16)
        swap(pair).start()

    lax.fori_loop(0, 2, late, None)

    def project(k, slot, first):
        t = (mine if k % 2 == 0 else theirs)[k // 2]
        wait_slot(slot)

        def body(n, _):
            r = _dot(t, W[slot, pl.ds(pl.multiple_of(1024 * n, 1024), 1024), :])
            y[n] = r if first else y[n] + r

        lax.fori_loop(0, NB, body, None)

    project(0, 6, True)
    swap(0).wait_recv()
    project(1, 7, False)
    project(2, 0, False)
    swap(1).wait_recv()
    wait_slot(1)

    def out_copies(n):
        at = pl.ds(pl.multiple_of(COLS * c + N * n, N), N)
        keep = pltpu.make_async_copy(yo.at[n, own_rows], y_hbm.at[:, at], ysem.at[n])
        give = pltpu.make_async_remote_copy(yo.at[n, their_rows], y_hbm.at[:, at], ysend.at[n], yrecv.at[n], {"sp": partner},
                                            pl.DeviceIdType.MESH)
        return keep, give

    t = theirs[1]

    def last(n, _):
        r = y[n] + _dot(t, W[1, pl.ds(pl.multiple_of(1024 * n, 1024), 1024), :])
        at = pl.ds(pl.multiple_of(COLS * c + N * n, N), N)
        yo[n] = (xr[:, at].astype(F32) + r).astype(BF16)
        keep, give = out_copies(n)
        give.start()
        keep.start()

    lax.fori_loop(0, NB, last, None)

    def finish(n, _):
        keep, give = out_copies(n)
        keep.wait()
        give.wait()

    lax.fori_loop(0, NB, finish, None)
    x_out.wait_send()
    for pair in range(2):
        swap(pair).wait_send()
        for half in range(2):
            @pl.when(chip != 3)
            def _():
                unit_copy(chip, pair, half, ksend.at[0, pair, half], chip).wait_send()

            @pl.when(chip == 0)
            def _():
                unit_copy(chip, pair, half, ksend.at[1, pair, half], chip).wait_send()

            @pl.when((chip == 3) | (chip == half + 1))
            def _():
                unit_copy(chip, pair, half, rsend.at[pair, half], chip).wait_send()


def solution(mesh):
    cos, sin = tables(4 * TOK)

    def step(x, gain, wq, wk, wv, wo):
        anywhere = pl.BlockSpec(memory_space=pl.ANY)
        dma = pltpu.SemaphoreType.DMA
        return pl.pallas_call(
            kernel,
            out_shape=jax.ShapeDtypeStruct((OWN, D), BF16),
            in_specs=[anywhere] * 8,
            out_specs=anywhere,
            scratch_shapes=[
                pltpu.VMEM((SLOTS, D, N), BF16),
                pltpu.VMEM((TOK, D), BF16),
                pltpu.VMEM((TOK, D), BF16),
                pltpu.VMEM((1, D), BF16),
                pltpu.VMEM((TOK, HEAD), F32),
                pltpu.VMEM((TOK, HEAD), F32),
                pltpu.VMEM((4, 4 * TOK, HEAD), BF16),
                pltpu.VMEM((4, 2, 2, 2, OWN, 2 * HEAD), BF16),
                pltpu.VMEM((4, HEAD + 8, 4 * TOK), F32),
                pltpu.VMEM((4, 1, 4 * TOK), F32),
                pltpu.VMEM((2, TOK, 1024), BF16),
                pltpu.VMEM((2, TOK, 1024), BF16),
                pltpu.VMEM((NB, TOK, N), F32),
                pltpu.VMEM((NB, TOK, N), BF16),
                dma((SLOTS,)), dma, dma, dma, dma((3,)), dma((2, 2, 2)), dma((4, 2, 2)), dma((2, 2)), dma((2,)), dma((2,)),
                dma((NB,)), dma((NB,)), dma((NB,)),
            ],
            compiler_params=pltpu.CompilerParams(collective_id=0, has_side_effects=True, vmem_limit_bytes=67043328),
        )(x, gain.reshape(1, D), wq, wk, wv, wo, jnp.asarray(cos), jnp.asarray(sin))

    tokens, whole = P(("dp", "sp"), None), P(None, None)
    return jax.shard_map(step, mesh=mesh, in_specs=(tokens, P(None), whole, whole, whole, whole), out_specs=tokens, check_vma=False)
```

```python
import functools

import jax
import jax.numpy as jnp
import numpy as np
from jax import lax
from jax.experimental import pallas as pl
from jax.experimental.pallas import tpu as pltpu
from jax.sharding import PartitionSpec as P

HEAD = 128
THETA = 10000
LOG2E = 1.4426950408889634
HIDDEN = -2e30
E = HEAD**-0.5 * LOG2E
F32, BF16 = jnp.float32, jnp.bfloat16

OWN = 128
TOK = 256
D = 5120
N = 512
COLS = D // 2
NB = COLS // N
SLOTS = 8
PIECE = 32
PIECES = OWN // PIECE


def tables(rows):
    half = HEAD // 2
    power = np.float32(THETA) ** (-np.arange(half, dtype=np.float32) / np.float32(half))
    angle = np.arange(rows, dtype=np.float32)[:, None] * power.astype(np.float32)
    cos, sin = np.cos(angle.astype(np.float32)), np.sin(angle.astype(np.float32))
    return np.concatenate([cos, cos], 1).astype(np.float32), np.concatenate([-sin, sin], 1).astype(np.float32)


def _dot(a, b, ca=1, cb=0):
    return lax.dot_general(a, b, (((ca,), (cb,)), ((), ())), preferred_element_type=F32)


def kernel(x_hbm, gain_hbm, wq, wk, wv, wo, cos_hbm, sin_hbm, y_out,
           W, xr, a, gain, gain8, cos, sin, q, kv, acc, top_s, mine, theirs, y, yo,
           wsem, xsem, xsend, xrecv, tsem, ksend, krecv, rsend, asend, arecv, ysend, yrecv):
    me = lax.axis_index("sp")
    chip, c = me // 2, me % 2
    partner = chip * 2 + (1 - c)

    def there(chip_to):
        return {"sp": chip_to * 2 + c}

    def load_kv(pair):
        for i in range(2):
            at = pl.multiple_of((4 * c + 2 * pair + i) * HEAD, HEAD)
            pltpu.make_async_copy(wk.at[:, pl.ds(at, HEAD)], W.at[pair, :, pl.ds(i * 256, HEAD)], wsem.at[pair]).start(priority=1)
            pltpu.make_async_copy(wv.at[:, pl.ds(at, HEAD)], W.at[pair, :, pl.ds(i * 256 + HEAD, HEAD)], wsem.at[pair]).start(priority=1)

    def load_q(s):
        at = pl.multiple_of(2048 * c + N * s, N)
        pltpu.make_async_copy(wq.at[:, pl.ds(at, N)], W.at[2 + s], wsem.at[2 + s]).start(priority=1)

    def load_o(k, slot):
        side = c if k % 2 == 0 else 1 - c
        row = pl.multiple_of(2048 * side + 1024 * (k // 2), 1024)
        for n in range(NB):
            at = pl.multiple_of(COLS * c + N * n, N)
            pltpu.make_async_copy(wo.at[pl.ds(row, 1024), pl.ds(at, N)], W.at[slot, pl.ds(1024 * n, 1024), :], wsem.at[slot]).start(priority=1)

    def wait_slot(s):
        pltpu.make_async_copy(W.at[s], W.at[s], wsem.at[s]).wait()

    own_rows = pl.ds(pl.multiple_of(c * OWN, OWN), OWN)
    their_rows = pl.ds(pl.multiple_of((1 - c) * OWN, OWN), OWN)

    def x_piece(i, first):
        return pl.ds(pl.multiple_of(first + i * PIECE, PIECE), PIECE)

    x_in = [pltpu.make_async_copy(x_hbm.at[i * PIECE : (i + 1) * PIECE], xr.at[x_piece(i, c * OWN)], xsem.at[i]) for i in range(PIECES)]
    for piece in x_in:
        piece.start()
    places = pl.ds(pl.multiple_of(chip * TOK, TOK), TOK)
    small = [pltpu.make_async_copy(gain_hbm, gain, tsem.at[0]),
             pltpu.make_async_copy(cos_hbm.at[places], cos, tsem.at[1]),
             pltpu.make_async_copy(sin_hbm.at[places], sin, tsem.at[2])]
    for s in small:
        s.start()
    load_kv(0)
    load_kv(1)
    for s in range(4):
        load_q(s)
    load_o(0, 6)
    load_o(1, 7)

    barrier = pltpu.get_barrier_semaphore()
    for peer in (partner, (chip + 1 - 2 * (chip % 2)) * 2 + c, (chip + 2) % 4 * 2 + c):
        pl.semaphore_signal(barrier, inc=1, device_id={"sp": peer}, device_id_type=pl.DeviceIdType.MESH)
    pl.semaphore_wait(barrier, 3)

    small[0].wait()
    gain8[...] = jnp.broadcast_to(gain[...].astype(F32)[None, :], (8, D))
    x_out = []
    for i in range(PIECES):
        x_in[i].wait()
        at = x_piece(i, c * OWN)
        x_out.append(pltpu.make_async_remote_copy(xr.at[at], xr.at[at], xsend.at[i], xrecv.at[i], {"sp": partner}, pl.DeviceIdType.MESH))
        x_out[i].start()

    def norm(first):
        def body(i, _):
            groups = [pl.ds(pl.multiple_of(first + i * 64 + n * 16, 16), 16) for n in range(4)]
            scales = []
            for rows in groups:
                total = jnp.zeros((16, HEAD), F32)
                for at in range(0, D, HEAD):
                    wide = xr[rows, at : at + HEAD].astype(F32)
                    total += wide * wide
                scales.append(lax.rsqrt(jnp.sum(total, -1, keepdims=True) * (1 / D) + 1e-6))
            for at in range(0, D, HEAD):
                g = jnp.concatenate([gain8[:, at : at + HEAD]] * 2, 0)
                for rows, scale in zip(groups, scales):
                    a[rows, at : at + HEAD] = (xr[rows, at : at + HEAD].astype(F32) * scale * g).astype(BF16)

        lax.fori_loop(0, OWN // 64, body, None)

    def turn(t, rows):
        t = t.astype(BF16).astype(F32)
        return (t * cos[rows, :] + pltpu.roll(t, 64, 1) * sin[rows, :]).astype(BF16)

    def unit_copy(j, pair, half, sem, chip_to):
        return pltpu.make_async_remote_copy(kv.at[j, pair, half], kv.at[j, pair, half], sem, krecv.at[j, pair, half],
                                            there(chip_to), pl.DeviceIdType.MESH)

    def make_kv(half, pair, detour=False):
        rows = pl.ds(pl.multiple_of(half * OWN, OWN), OWN)
        r = _dot(a[rows, :], W[pair])
        for i in range(2):
            kv[chip, pair, half, i, :, :HEAD] = turn(r[:, i * 256 : i * 256 + HEAD], rows)
            kv[chip, pair, half, i, :, HEAD:] = r[:, i * 256 + HEAD : (i + 1) * 256].astype(BF16)

        @pl.when(chip != 3)
        def _():
            unit_copy(chip, pair, half, ksend.at[0, pair, half], jnp.where(chip == 0, 1, 3)).start()

        @pl.when(chip == 0)
        def _():
            unit_copy(chip, pair, half, ksend.at[1, pair, half], 2).start()

        if detour:
            @pl.when(chip == 1)
            def _():
                unit_copy(chip, pair, half, ksend.at[1, pair, half], 0).start()

    norm(c * OWN)
    small[1].wait()
    small[2].wait()
    wait_slot(0)
    make_kv(c, 0)
    for piece in x_out:
        piece.wait_recv()
    norm((1 - c) * OWN)
    wait_slot(1)
    make_kv(c, 1)
    make_kv(1 - c, 0)
    make_kv(1 - c, 1, True)
    load_o(2, 0)
    load_o(3, 1)

    def pass_on(half, pair, by=3):
        @pl.when(chip == by)
        def _():
            move = unit_copy(1, pair, half, rsend.at[pair, half], 2)
            move.wait_recv()
            move.start()

    for s in range(0, 4, 2):
        wait_slot(2 + s)
        wait_slot(3 + s)
        for t in (s, s + 1):
            r = _dot(a[...], W[2 + t])
            for g in range(4):
                q[t, g * TOK : (g + 1) * TOK, :] = turn(r[:, g * HEAD : (g + 1) * HEAD], pl.ds(0, TOK))
        pass_on(c, s // 2)
    pass_on(1 - c, 0)
    pass_on(1 - c, 1, 0)

    def relay(pair):
        for p in (1, 2):
            @pl.when(chip == p)
            def _():
                move = unit_copy(0, pair, p - 1, rsend.at[pair, p - 1], 3)
                move.wait_recv()
                move.start()

    relay(0)

    def attend(j, pair, first):
        mask = None
        if first:
            mask = lax.broadcasted_iota(jnp.int32, (TOK, TOK), 0) <= lax.broadcasted_iota(jnp.int32, (TOK, TOK), 1)
        for i in range(2):
            h = 2 * pair + i
            keys = jnp.concatenate([kv[j, pair, t, i, :, :HEAD] for t in range(2)], 0)
            values = jnp.concatenate([kv[j, pair, t, i, :, HEAD:] for t in range(2)], 0)
            vt = jnp.concatenate([values.T, jnp.ones((8, TOK), BF16)], 0)
            scores = [_dot(keys, q[h, g * TOK : (g + 1) * TOK, :], 1, 1) for g in range(4)]
            for g, s in enumerate(scores):
                at = slice(g * TOK, (g + 1) * TOK)
                if first:
                    s = jnp.where(mask, s, HIDDEN)
                    top = s.max(axis=0, keepdims=True)
                    p = jnp.exp2((s - top) * E).astype(BF16)
                    acc[h, :, at] = _dot(vt, p)
                else:
                    old = top_s[h, :, at]
                    top = jnp.maximum(old, s.max(axis=0, keepdims=True))
                    p = jnp.exp2((s - top) * E).astype(BF16)
                    acc[h, :, at] = acc[h, :, at] * jnp.exp2((old - top) * E) + _dot(vt, p)
                top_s[h, :, at] = top

    def wait_units(j, pair):
        for half in range(2):
            @pl.when(jnp.logical_not(((j == 0) & (chip == half + 1)) | ((j == 1) & (chip == 3) & ((pair == 0) | (half == c)))))
            def _():
                unit_copy(j, pair, half, ksend.at[0, pair, half], chip).wait_recv()

    lax.fori_loop(0, 2, lambda pair, _: attend(chip, pair, True), None)
    relay(1)

    def early(t, _):
        s, pair = t // 2, t % 2
        j = jnp.where(chip == 3, 1 + s, 0)
        wait_units(j, pair)

        attend(j, pair, False)

    lax.fori_loop(0, 2 * jnp.maximum(chip - 1, 0), early, None)

    def swap(pair):
        return pltpu.make_async_remote_copy(mine.at[pair], theirs.at[pair], asend.at[pair], arecv.at[pair], {"sp": partner},
                                            pl.DeviceIdType.MESH)

    def late(pair, _):
        @pl.when(chip > 0)
        def _():
            j = jnp.where(chip == 2, 1, 0)
            wait_units(j, pair)
            attend(j, pair, False)

        for i in range(2):
            h = 2 * pair + i
            for g in range(4):
                at = slice(g * TOK, (g + 1) * TOK)
                out = acc[h, :HEAD, at] * (1 / acc[h, HEAD : HEAD + 1, at])
                mine[pair, :, (4 * i + g) * HEAD : (4 * i + g + 1) * HEAD] = out.T.astype(BF16)
        swap(pair).start()

    lax.fori_loop(0, 2, late, None)

    def blocks(slot, n):
        return W[slot, 1024 * n : 1024 * (n + 1), :]

    def out_copy(n):
        at = pl.ds(pl.multiple_of(COLS * c + N * n, N), N)
        return pltpu.make_async_remote_copy(yo.at[n, their_rows], y_out.at[:, at], ysend.at[n], yrecv.at[n], {"sp": partner},
                                            pl.DeviceIdType.MESH)

    wait_slot(6)
    swap(0).wait_recv()
    wait_slot(7)
    for n in range(NB):
        y[n] = _dot(mine[0], blocks(6, n)) + _dot(theirs[0], blocks(7, n))
    wait_slot(0)
    wait_slot(1)
    swap(1).wait_recv()
    for n in range(NB):
        r = y[n] + (_dot(mine[1], blocks(0, n)) + _dot(theirs[1], blocks(1, n)))
        at = pl.ds(pl.multiple_of(COLS * c + N * n, N), N)
        yo[n] = (xr[:, at].astype(F32) + r).astype(BF16)
        out_copy(n).start()
        y_out[:, at] = yo[n, own_rows]

    def finish(n, _):
        out_copy(n).wait()

    lax.fori_loop(0, NB, finish, None)
    for piece in x_out:
        piece.wait_send()
    for pair in range(2):
        swap(pair).wait_send()
        for half in range(2):
            @pl.when(chip != 3)
            def _():
                unit_copy(chip, pair, half, ksend.at[0, pair, half], chip).wait_send()

            @pl.when(chip == 0)
            def _():
                unit_copy(chip, pair, half, ksend.at[1, pair, half], chip).wait_send()

            last = (pair == 1) & (half != c)

            @pl.when((chip == half + 1) | ((chip == 3) & jnp.logical_not(last)) | ((chip == 0) & last))
            def _():
                unit_copy(chip, pair, half, rsend.at[pair, half], chip).wait_send()

            @pl.when((chip == 1) & last)
            def _():
                unit_copy(chip, pair, half, ksend.at[1, pair, half], chip).wait_send()


def solution(mesh):
    cos, sin = tables(4 * TOK)

    def step(x, gain, wq, wk, wv, wo):
        anywhere = pl.BlockSpec(memory_space=pl.ANY)
        dma = pltpu.SemaphoreType.DMA
        return pl.pallas_call(
            kernel,
            out_shape=pltpu.VMEM((OWN, D), BF16),
            in_specs=[anywhere] * 8,
            out_specs=pl.BlockSpec(memory_space=pltpu.VMEM),
            scratch_shapes=[
                pltpu.VMEM((SLOTS, D, N), BF16),
                pltpu.VMEM((TOK, D), BF16),
                pltpu.VMEM((TOK, D), BF16),
                pltpu.VMEM((D,), BF16),
                pltpu.VMEM((8, D), F32),
                pltpu.VMEM((TOK, HEAD), F32),
                pltpu.VMEM((TOK, HEAD), F32),
                pltpu.VMEM((4, 4 * TOK, HEAD), BF16),
                pltpu.VMEM((4, 2, 2, 2, OWN, 2 * HEAD), BF16),
                pltpu.VMEM((4, HEAD + 8, 4 * TOK), F32),
                pltpu.VMEM((4, 1, 4 * TOK), F32),
                pltpu.VMEM((2, TOK, 1024), BF16),
                pltpu.VMEM((2, TOK, 1024), BF16),
                pltpu.VMEM((NB, TOK, N), F32),
                pltpu.VMEM((NB, TOK, N), BF16),
                dma((SLOTS,)), dma((PIECES,)), dma((PIECES,)), dma((PIECES,)), dma((3,)), dma((2, 2, 2)), dma((4, 2, 2)), dma((2, 2)), dma((2,)), dma((2,)),
                dma((NB,)), dma((NB,)),
            ],
            compiler_params=pltpu.CompilerParams(collective_id=0, has_side_effects=True, vmem_limit_bytes=62 * 2**20),
        )(x, gain, wq, wk, wv, wo, jnp.asarray(cos), jnp.asarray(sin))

    tokens, whole = P(("dp", "sp"), None), P(None, None)
    return jax.shard_map(step, mesh=mesh, in_specs=(tokens, P(None), whole, whole, whole, whole), out_specs=tokens, check_vma=False)
```

```python
import functools

import jax
import jax.numpy as jnp
import numpy as np
from jax import lax
from jax.experimental import pallas as pl
from jax.experimental.pallas import tpu as pltpu
from jax.sharding import PartitionSpec as P

HEAD = 128
THETA = 10000
LOG2E = 1.4426950408889634
HIDDEN = -2e30
E = HEAD**-0.5 * LOG2E
F32, BF16 = jnp.float32, jnp.bfloat16

OWN = 128
TOK = 256
D = 5120
N = 512
COLS = D // 2
NB = COLS // N
SLOTS = 8
PIECE = 32
PIECES = OWN // PIECE


def tables(rows):
    half = HEAD // 2
    power = np.float32(THETA) ** (-np.arange(half, dtype=np.float32) / np.float32(half))
    angle = np.arange(rows, dtype=np.float32)[:, None] * power.astype(np.float32)
    cos, sin = np.cos(angle.astype(np.float32)), np.sin(angle.astype(np.float32))
    return np.concatenate([cos, sin], 1).astype(np.float32)


def _dot(a, b, ca=1, cb=0):
    return lax.dot_general(a, b, (((ca,), (cb,)), ((), ())), preferred_element_type=F32)


def kernel(x_hbm, gain_hbm, wq, wk, wv, wo, turns_hbm, y_out,
           W, xr, a, gain, gain8, cos, sin, q, kv, acc, top_s, mine, theirs, y, yo,
           wsem, kvsem, xsem, tsem, xsend, xrecv, nsend, nrecv, ksend, krecv, rsend, asend, arecv, ysend, yrecv):
    me = lax.axis_index("sp")
    chip, c = me // 2, me % 2
    partner = {"sp": chip * 2 + (1 - c)}
    mesh_id = pl.DeviceIdType.MESH

    def there(chip_to):
        return {"sp": chip_to * 2 + c}

    def load_kv(h):
        at = pl.multiple_of((4 * c + h) * HEAD, HEAD)
        for n, w in enumerate((wk, wv)):
            to = W.at[h // 2, :, pl.ds((h % 2) * 2 * HEAD + n * HEAD, HEAD)]
            pltpu.make_async_copy(w.at[:, pl.ds(at, HEAD)], to, kvsem.at[h]).start(priority=1)

    def wait_kv(h):
        to = W.at[h // 2, :, pl.ds((h % 2) * 2 * HEAD, 2 * HEAD)]
        pltpu.make_async_copy(to, to, kvsem.at[h]).wait()

    def load_q(s):
        at = pl.multiple_of(2048 * c + N * s, N)
        pltpu.make_async_copy(wq.at[:, pl.ds(at, N)], W.at[2 + s], wsem.at[2 + s]).start(priority=1)

    def load_o(k, slot):
        side = c if k % 2 == 0 else 1 - c
        row = pl.multiple_of(2048 * side + 1024 * (k // 2), 1024)
        for n in range(NB):
            at = pl.multiple_of(COLS * c + N * n, N)
            to = W.at[slot, pl.ds(1024 * n, 1024), :]
            pltpu.make_async_copy(wo.at[pl.ds(row, 1024), pl.ds(at, N)], to, wsem.at[slot]).start(priority=1)

    def wait_slot(s):
        pltpu.make_async_copy(W.at[s], W.at[s], wsem.at[s]).wait()

    own_rows = pl.ds(pl.multiple_of(c * OWN, OWN), OWN)
    their_rows = pl.ds(pl.multiple_of((1 - c) * OWN, OWN), OWN)
    own_columns = pl.ds(pl.multiple_of(COLS * c, N), COLS)
    their_columns = pl.ds(pl.multiple_of(COLS * (1 - c), N), COLS)

    def rows_of(half, i):
        return pl.ds(pl.multiple_of(half * OWN + i * PIECE, PIECE), PIECE)

    x_in = [pltpu.make_async_copy(x_hbm.at[i * PIECE : (i + 1) * PIECE], xr.at[rows_of(c, i)], xsem.at[i]) for i in range(PIECES)]
    gain_in = pltpu.make_async_copy(gain_hbm, gain, tsem.at[0])
    gain_in.start()
    for piece in x_in:
        piece.start()
    places = pl.ds(pl.multiple_of(chip * TOK, TOK), TOK)
    turns_in = pltpu.make_async_copy(turns_hbm.at[places], cos, tsem.at[1])
    turns_in.start()
    for h in range(4):
        load_kv(h)
    for s in range(4):
        load_q(s)
    load_o(0, 6)
    load_o(1, 7)

    barrier = pltpu.get_barrier_semaphore()
    for peer in (partner, there(chip + 1 - 2 * (chip % 2)), there((chip + 2) % 4)):
        pl.semaphore_signal(barrier, inc=1, device_id=peer, device_id_type=mesh_id)
    pl.semaphore_wait(barrier, 3)

    gain_in.wait()
    gain8[...] = jnp.broadcast_to(gain[...].astype(F32)[None, :], (8, D))

    def norm_copy(i):
        return pltpu.make_async_remote_copy(a.at[rows_of(c, i)], a.at[rows_of(c, i)], nsend.at[i], nrecv.at[i], partner, mesh_id)

    for i in range(PIECES):
        x_in[i].wait()
        first = c * OWN + i * PIECE
        groups = [pl.ds(pl.multiple_of(first + n * 16, 16), 16) for n in range(PIECE // 16)]
        scales = []
        for rows in groups:
            total = jnp.zeros((16, HEAD), F32)
            for at in range(0, D, HEAD):
                wide = xr[rows, at : at + HEAD].astype(F32)
                total += wide * wide
            scales.append(lax.rsqrt(jnp.sum(total, -1, keepdims=True) * (1 / D) + 1e-6))
        for at in range(0, D, HEAD):
            g = jnp.concatenate([gain8[:, at : at + HEAD]] * 2, 0)
            for rows, scale in zip(groups, scales):
                a[rows, at : at + HEAD] = (xr[rows, at : at + HEAD].astype(F32) * scale * g).astype(BF16)
        norm_copy(i).start()

    turns_in.wait()
    both = cos[...]
    other = pltpu.roll(both, 64, 1)
    low = lax.broadcasted_iota(jnp.int32, (TOK, HEAD), 1) < HEAD // 2
    cos[...] = jnp.where(low, both, other)
    sin[...] = jnp.where(low, -other, both)

    def turn(t, rows):
        t = t.astype(BF16).astype(F32)
        return (t * cos[rows, :] + pltpu.roll(t, 64, 1) * sin[rows, :]).astype(BF16)

    def unit_copy(j, h, half, sem, chip_to):
        unit = kv.at[j, h, half]
        return pltpu.make_async_remote_copy(unit, unit, sem, krecv.at[j, h, half], there(chip_to), mesh_id)

    def make_kv(rows, halves, heads):
        lo = (heads[0] % 2) * 2 * HEAD
        r = _dot(a[rows, :], W[heads[0] // 2, :, lo : lo + len(heads) * 2 * HEAD])
        for i, h in enumerate(heads):
            keys = turn(r[:, i * 256 : i * 256 + HEAD], rows)
            values = r[:, i * 256 + HEAD : (i + 1) * 256].astype(BF16)
            for n, half in enumerate(halves):
                kv[chip, h, half, :, :HEAD] = keys[n * OWN : (n + 1) * OWN]
                kv[chip, h, half, :, HEAD:] = values[n * OWN : (n + 1) * OWN]

    def send(half, h, chips=(0, 1, 2)):
        if 0 in chips:
            @pl.when(chip == 0)
            def _():
                for n in range(2):
                    unit_copy(chip, h, half, ksend.at[n, h, half], n + 1).start()

        if 1 in chips:
            @pl.when((chip == 1) | (chip == 2))
            def _():
                unit_copy(chip, h, half, ksend.at[0, h, half], 3).start()

    def pass_on(half, h, by=3):
        @pl.when(chip == by)
        def _():
            move = unit_copy(1, h, half, rsend.at[h, half], 2)
            move.wait_recv()
            move.start()

    def relay(h):
        for p in (1, 2):
            @pl.when(chip == p)
            def _():
                move = unit_copy(0, h, p - 1, rsend.at[h, p - 1], 3)
                move.wait_recv()
                move.start()

    for h in range(2):
        wait_kv(h)
        make_kv(own_rows, (c,), (h,))
        send(c, h)
    for i in range(PIECES):
        norm_copy(i).wait_recv()
    make_kv(their_rows, (1 - c,), (0, 1))
    send(1 - c, 0)
    send(1 - c, 1)
    wait_kv(2)
    wait_kv(3)
    make_kv(pl.ds(0, TOK), (0, 1), (2, 3))
    for h in (2, 3):
        send(c, h)
    for h in (2, 3):
        send(1 - c, h, (0,))

        @pl.when(chip == 1)
        def _():
            unit_copy(chip, h, 1 - c, ksend.at[1, h, 1 - c], 0).start()

    load_o(2, 0)
    load_o(3, 1)
    x_out = pltpu.make_async_remote_copy(x_hbm.at[:, their_columns], xr.at[own_rows, their_columns], xsend, xrecv, partner, mesh_id)
    x_out.start()
    pass_on(c, 0)

    for s in range(4):
        wait_slot(2 + s)
        r = _dot(a[...], W[2 + s])
        for g in range(4):
            q[s, g * TOK : (g + 1) * TOK, :] = turn(r[:, g * HEAD : (g + 1) * HEAD], pl.ds(0, TOK))
        if s == 0:
            pass_on(c, 1)
        if s == 1:
            pass_on(1 - c, 0)
            relay(0)
        if s == 2:
            pass_on(1 - c, 1)
            relay(1)
            send(1 - c, 2, (1,))
            send(1 - c, 3, (1,))
    pass_on(c, 2)
    pass_on(1 - c, 2, 0)
    pass_on(1 - c, 3, 0)

    def attend(heads, js, first=False):
        mask = None
        if first:
            mask = lax.broadcasted_iota(jnp.int32, (TOK, TOK), 0) <= lax.broadcasted_iota(jnp.int32, (TOK, TOK), 1)
        units = [(h, slice(g * TOK, (g + 1) * TOK)) for h in heads for g in range(4)]
        chunks, scores, weights, keeps = {}, {}, {}, {}

        def score(n):
            h, at = units[n]
            if h not in chunks:
                chunks[h] = []
                for j in js:
                    values = jnp.concatenate([kv[j, h, t, :, HEAD:] for t in range(2)], 0)
                    chunks[h].append((jnp.concatenate([kv[j, h, t, :, :HEAD] for t in range(2)], 0),
                                      jnp.concatenate([values.T, jnp.ones((8, TOK), BF16)], 0)))
            scores[n] = [_dot(keys, q[h, at, :], 1, 1) for keys, _ in chunks[h]]

        def weigh(n):
            h, at = units[n]
            some = scores.pop(n)
            if first:
                some = [jnp.where(mask, s, HIDDEN) for s in some]
            tops = [s.max(axis=0, keepdims=True) for s in some]
            top = functools.reduce(jnp.maximum, tops)
            if not first:
                old = top_s[h, :, at]
                top = jnp.maximum(old, top)
                keeps[n] = jnp.exp2((old - top) * E)
            top_s[h, :, at] = top
            weights[n] = [jnp.exp2((s - top) * E).astype(BF16) for s in some]

        def add(n):
            h, at = units[n]
            parts = [_dot(vt, p) for p, (_, vt) in zip(weights.pop(n), chunks[h])]
            total = functools.reduce(jnp.add, parts)
            acc[h, :, at] = total if first else acc[h, :, at] * keeps.pop(n) + total

        ahead = 4 if len(js) == 1 else 2
        for n in range(len(units) + ahead + 1):
            if n < len(units):
                score(n)
            if 0 <= n - ahead < len(units):
                weigh(n - ahead)
            if 0 <= n - ahead - 1:
                add(n - ahead - 1)

    def wait_units(j, heads):
        for h in heads:
            for t in range(2):
                @pl.when(jnp.logical_not(((j == 0) & (chip == t + 1)) | ((j == 1) & (chip == 3) & ((h < 2) | (c == t)))))
                def _():
                    unit_copy(j, h, t, ksend.at[0, h, t], chip).wait_recv()

    attend(range(4), [chip], True)
    pass_on(c, 3)

    def early(pair):
        heads = (2 * pair, 2 * pair + 1)

        @pl.when(chip == 3)
        def _():
            wait_units(1, heads)
            wait_units(2, heads)
            attend(heads, [1, 2])

        @pl.when(chip == 2)
        def _():
            wait_units(0, heads)
            attend(heads, [0])

    def swap(pair):
        return pltpu.make_async_remote_copy(mine.at[pair], theirs.at[pair], asend.at[pair], arecv.at[pair], partner, mesh_id)

    def late(pair):
        heads = (2 * pair, 2 * pair + 1)

        @pl.when(chip > 0)
        def _():
            j = jnp.where(chip == 2, 1, 0)
            wait_units(j, heads)
            attend(heads, [j])

        for i, h in enumerate(heads):
            for g in range(4):
                at = slice(g * TOK, (g + 1) * TOK)
                out = acc[h, :HEAD, at] * (1 / acc[h, HEAD : HEAD + 1, at])
                mine[pair, :, (4 * i + g) * HEAD : (4 * i + g + 1) * HEAD] = out.astype(BF16).T
        swap(pair).start()

    def blocks(slot, n):
        return W[slot, 1024 * n : 1024 * (n + 1), :]

    early(0)
    relay(2)
    late(0)
    relay(3)
    wait_slot(6)
    for n in range(NB):
        y[n] = _dot(mine[0], blocks(6, n))
    early(1)
    swap(0).wait_recv()
    wait_slot(7)
    for n in range(NB):
        y[n] += _dot(theirs[0], blocks(7, n))
    late(1)
    wait_slot(0)
    for n in range(NB):
        y[n] += _dot(mine[1], blocks(0, n))
    wait_slot(1)
    x_out.wait_recv()
    swap(1).wait_recv()

    def out_copy(n):
        at = pl.ds(pl.multiple_of(COLS * c + N * n, N), N)
        return pltpu.make_async_remote_copy(yo.at[n], y_out.at[:, at], ysend.at[n], yrecv.at[n], partner, mesh_id)

    def result(n, rows):
        at = pl.ds(pl.multiple_of(COLS * c + N * n, N), N)
        r = y[n, rows] + _dot(theirs[1, rows], blocks(1, n))
        return (xr[rows, at].astype(F32) + r).astype(BF16), at

    for group in ((0, 1, 2), (3, 4)):
        for n in group:
            yo[n], _ = result(n, their_rows)
        for n in group:
            out_copy(n).start()
    for n in range(NB):
        part, at = result(n, own_rows)
        y_out[:, at] = part

    for n in range(NB):
        out_copy(n).wait()
    x_out.wait_send()
    for i in range(PIECES):
        norm_copy(i).wait_send()
    for pair in range(2):
        swap(pair).wait_send()

    def sent(h, _):
        for t in range(2):
            detour = (h >= 2) & (c != t)

            @pl.when(chip != 3)
            def _():
                unit_copy(chip, h, t, ksend.at[0, h, t], chip).wait_send()

            @pl.when((chip == 0) | ((chip == 1) & detour))
            def _():
                unit_copy(chip, h, t, ksend.at[1, h, t], chip).wait_send()

            @pl.when((chip == t + 1) | ((chip == 3) & jnp.logical_not(detour)) | ((chip == 0) & detour))
            def _():
                unit_copy(chip, h, t, rsend.at[h, t], chip).wait_send()

    lax.fori_loop(0, 4, sent, None)


def solution(mesh):
    turns = tables(4 * TOK)

    def step(x, gain, wq, wk, wv, wo):
        anywhere = pl.BlockSpec(memory_space=pl.ANY)
        dma = pltpu.SemaphoreType.DMA
        return pl.pallas_call(
            kernel,
            out_shape=pltpu.VMEM((OWN, D), BF16),
            in_specs=[anywhere] * 7,
            out_specs=pl.BlockSpec(memory_space=pltpu.VMEM),
            scratch_shapes=[
                pltpu.VMEM((SLOTS, D, N), BF16),
                pltpu.VMEM((TOK, D), BF16),
                pltpu.VMEM((TOK, D), BF16),
                pltpu.VMEM((D,), BF16),
                pltpu.VMEM((8, D), F32),
                pltpu.VMEM((TOK, HEAD), F32),
                pltpu.VMEM((TOK, HEAD), F32),
                pltpu.VMEM((4, 4 * TOK, HEAD), BF16),
                pltpu.VMEM((4, 4, 2, OWN, 2 * HEAD), BF16),
                pltpu.VMEM((4, HEAD + 8, 4 * TOK), F32),
                pltpu.VMEM((4, 1, 4 * TOK), F32),
                pltpu.VMEM((2, TOK, 1024), BF16),
                pltpu.VMEM((2, TOK, 1024), BF16),
                pltpu.VMEM((NB, TOK, N), F32),
                pltpu.VMEM((NB, OWN, N), BF16),
                dma((SLOTS,)), dma((4,)), dma((PIECES,)), dma((2,)), dma, dma, dma((PIECES,)), dma((PIECES,)),
                dma((2, 4, 2)), dma((4, 4, 2)), dma((4, 2)), dma((2,)), dma((2,)), dma((NB,)), dma((NB,)),
            ],
            compiler_params=pltpu.CompilerParams(collective_id=0, has_side_effects=True, vmem_limit_bytes=62 * 2**20),
        )(x, gain, wq, wk, wv, wo, jnp.asarray(turns))

    tokens, whole = P(("dp", "sp"), None), P(None, None)
    return jax.shard_map(step, mesh=mesh, in_specs=(tokens, P(None), whole, whole, whole, whole), out_specs=tokens, check_vma=False)
```

```python
import functools

import jax
import jax.numpy as jnp
import numpy as np
from jax import lax
from jax.experimental import pallas as pl
from jax.experimental.pallas import tpu as pltpu
from jax.sharding import PartitionSpec as P

HEAD = 128
THETA = 10000
LOG2E = 1.4426950408889634
HIDDEN = -2e30
E = HEAD**-0.5 * LOG2E
F32, BF16 = jnp.float32, jnp.bfloat16

OWN = 128
TOK = 256
D = 5120
N = 512
COLS = D // 2
HALF = D // 2
NB = COLS // N
SLOTS = 8
PIECE = 32
PIECES = OWN // PIECE


def tables(rows):
    half = HEAD // 2
    power = np.float32(THETA) ** (-np.arange(half, dtype=np.float32) / np.float32(half))
    angle = np.arange(rows, dtype=np.float32)[:, None] * power.astype(np.float32)
    cos, sin = np.cos(angle.astype(np.float32)), np.sin(angle.astype(np.float32))
    return np.concatenate([cos, sin], 1).astype(np.float32)


def _dot(a, b, ca=1, cb=0):
    return lax.dot_general(a, b, (((ca,), (cb,)), ((), ())), preferred_element_type=F32)


def kernel(x_hbm, gain_hbm, wq, wk, wv, wo, turns_hbm, y_out,
           W, xr, a, gain, gain8, cos, sin, q, kv, acc, top_s, mine, theirs, y, yo,
           wsem, kvsem, xsem, tsem, xsend, xrecv, nsend, nrecv, ksend, krecv, rsend, asend, arecv, ysend, yrecv):
    me = lax.axis_index("sp")
    chip, c = me // 2, me % 2
    partner = {"sp": chip * 2 + (1 - c)}
    mesh_id = pl.DeviceIdType.MESH

    def there(chip_to):
        return {"sp": chip_to * 2 + c}

    def load_kv(h):
        at = pl.multiple_of((4 * c + h) * HEAD, HEAD)
        for part in range(2):
            rows = pl.ds(part * HALF, HALF)
            for n, w in enumerate((wk, wv)):
                to = W.at[h // 2, rows, pl.ds((h % 2) * 2 * HEAD + n * HEAD, HEAD)]
                sem = kvsem.at[part if h == 0 else min(h, 2) + 1]
                pltpu.make_async_copy(w.at[rows, pl.ds(at, HEAD)], to, sem).start(priority=1)

    def wait_kv(n):
        to = (W.at[0, pl.ds(0, HALF), pl.ds(0, 256)], W.at[0, pl.ds(HALF, HALF), pl.ds(0, 256)], W.at[0, :, pl.ds(256, 256)], W.at[1])[n]
        pltpu.make_async_copy(to, to, kvsem.at[n]).wait()

    def slot_sem(s):
        return wsem.at[s - 2] if s >= 2 else kvsem.at[s]

    def load_q(s):
        at = pl.multiple_of(2048 * c + N * s, N)
        pltpu.make_async_copy(wq.at[:, pl.ds(at, N)], W.at[2 + s], slot_sem(2 + s)).start(priority=1)

    def load_o(k, slot):
        side = c if k % 2 == 0 else 1 - c
        row = pl.multiple_of(2048 * side + 1024 * (k // 2), 1024)
        for n in range(NB):
            at = pl.multiple_of(COLS * c + N * n, N)
            to = W.at[slot, pl.ds(1024 * n, 1024), :]
            pltpu.make_async_copy(wo.at[pl.ds(row, 1024), pl.ds(at, N)], to, slot_sem(slot)).start(priority=1)

    def wait_slot(s):
        pltpu.make_async_copy(W.at[s], W.at[s], slot_sem(s)).wait()

    own_rows = pl.ds(pl.multiple_of(c * OWN, OWN), OWN)
    their_rows = pl.ds(pl.multiple_of((1 - c) * OWN, OWN), OWN)
    own_columns = pl.ds(pl.multiple_of(COLS * c, N), COLS)
    their_columns = pl.ds(pl.multiple_of(COLS * (1 - c), N), COLS)

    def rows_of(half, i):
        return pl.ds(pl.multiple_of(half * OWN + i * PIECE, PIECE), PIECE)

    x_in = [pltpu.make_async_copy(x_hbm.at[i * PIECE : (i + 1) * PIECE], xr.at[rows_of(c, i)], xsem.at[i]) for i in range(PIECES)]
    gain_in = pltpu.make_async_copy(gain_hbm, gain, tsem.at[0])
    gain_in.start()
    for piece in x_in:
        piece.start()
    places = pl.ds(pl.multiple_of(chip * TOK, TOK), TOK)
    turns_in = pltpu.make_async_copy(turns_hbm.at[places], cos, tsem.at[1])
    turns_in.start()
    for h in range(4):
        load_kv(h)
    for s in range(4):
        load_q(s)
    load_o(0, 6)
    load_o(1, 7)

    barrier = pltpu.get_barrier_semaphore()
    for peer in (partner, there(chip + 1 - 2 * (chip % 2)), there((chip + 2) % 4)):
        pl.semaphore_signal(barrier, inc=1, device_id=peer, device_id_type=mesh_id)
    pl.semaphore_wait(barrier, 3)

    gain_in.wait()
    gain8[...] = jnp.broadcast_to(gain[...].astype(F32)[None, :], (8, D))

    def norm_copy(i):
        part = a.at[rows_of(c, i), pl.ds(0, HALF)] if i < PIECES else a.at[own_rows, pl.ds(HALF, HALF)]
        return pltpu.make_async_remote_copy(part, part, nsend, nrecv.at[i // PIECES], partner, mesh_id)

    for i in range(PIECES):
        x_in[i].wait()
        first = c * OWN + i * PIECE
        groups = [pl.ds(pl.multiple_of(first + n * 16, 16), 16) for n in range(PIECE // 16)]
        scales = []
        for rows in groups:
            total = jnp.zeros((16, HEAD), F32)
            for at in range(0, D, HEAD):
                wide = xr[rows, at : at + HEAD].astype(F32)
                total += wide * wide
            scales.append(lax.rsqrt(jnp.sum(total, -1, keepdims=True) * (1 / D) + 1e-6))
        for at in range(0, D, HEAD):
            g = jnp.concatenate([gain8[:, at : at + HEAD]] * 2, 0)
            for rows, scale in zip(groups, scales):
                a[rows, at : at + HEAD] = (xr[rows, at : at + HEAD].astype(F32) * scale * g).astype(BF16)
        norm_copy(i).start()
    norm_copy(PIECES).start()

    turns_in.wait()
    both = cos[...]
    other = pltpu.roll(both, 64, 1)
    low = lax.broadcasted_iota(jnp.int32, (TOK, HEAD), 1) < HEAD // 2
    cos[...] = jnp.where(low, both, other)
    sin[...] = jnp.where(low, -other, both)

    def turn(t, rows):
        t = t.astype(BF16).astype(F32)
        return (t * cos[rows, :] + pltpu.roll(t, 64, 1) * sin[rows, :]).astype(BF16)

    def unit_copy(j, h, half, sem, chip_to, count):
        unit = kv.at[j, h, half]
        return pltpu.make_async_remote_copy(unit, unit, sem, krecv.at[count], there(chip_to), mesh_id)

    def arrived(units, count):
        pltpu.make_async_copy(units, units, krecv.at[count]).wait()

    def make_kv(rows, halves, heads, gates):
        lo = (heads[0] % 2) * 2 * HEAD
        columns = slice(lo, lo + len(heads) * 2 * HEAD)
        gates[0]()
        r = _dot(a[rows, :HALF], W[heads[0] // 2, :HALF, columns])
        gates[1]()
        r += _dot(a[rows, HALF:], W[heads[0] // 2, HALF:, columns])
        for i, h in enumerate(heads):
            keys = turn(r[:, i * 256 : i * 256 + HEAD], rows)
            values = r[:, i * 256 + HEAD : (i + 1) * 256].astype(BF16)
            for n, half in enumerate(halves):
                kv[chip, h, half, :, :HEAD] = keys[n * OWN : (n + 1) * OWN]
                kv[chip, h, half, :, HEAD:] = values[n * OWN : (n + 1) * OWN]

    def send(own, h, chips=(0, 1, 2)):
        half = c if own else 1 - c
        if 0 in chips:
            @pl.when(chip == 0)
            def _():
                for n in range(2):
                    unit_copy(chip, h, half, ksend.at[n], n + 1, jnp.where(half == n, h, 4 + h // 2)).start()

        if 1 in chips:
            @pl.when((chip == 1) | (chip == 2))
            def _():
                count = jnp.where(chip == 2, 2 + h // 2, 4 + h if own else min(8 + h, 10))
                unit_copy(chip, h, half, ksend.at[0], 3, count).start()

    def pass_on(own, h, by=3):
        half = c if own else 1 - c

        @pl.when(chip == by)
        def _():
            arrived(kv.at[1, h, half], h - 2 if by == 0 else 4 + h if own else 8 + h)
            unit_copy(1, h, half, rsend, 2, 6 + h // 2).start()

    def relay(h):
        for p in (1, 2):
            @pl.when(chip == p)
            def _():
                arrived(kv.at[0, h, p - 1], h)
                unit_copy(0, h, p - 1, rsend, 3, h // 2).start()

    def gate(*waits):
        def run():
            for wait in waits:
                wait()
        return run

    make_kv(own_rows, (c,), (0,), (gate(functools.partial(wait_kv, 0)), gate(functools.partial(wait_kv, 1))))
    send(True, 0)
    make_kv(own_rows, (c,), (1,), (gate(functools.partial(wait_kv, 2)), gate()))
    send(True, 1)
    def theirs_here(n):
        part = a.at[their_rows, pl.ds(n * HALF, HALF)]
        pltpu.make_async_copy(part, part, nrecv.at[n]).wait()

    halves = gate(functools.partial(theirs_here, 0)), gate(functools.partial(theirs_here, 1))
    make_kv(their_rows, (1 - c,), (0, 1), halves)
    send(False, 0)
    send(False, 1)
    make_kv(pl.ds(0, TOK), (0, 1), (2, 3), (gate(functools.partial(wait_kv, 3)), gate()))
    for h in (2, 3):
        send(True, h)
    for h in (2, 3):
        send(False, h, (0,))

        @pl.when(chip == 1)
        def _():
            unit_copy(chip, h, 1 - c, ksend.at[1], 0, h - 2).start()

    load_o(2, 0)
    load_o(3, 1)
    x_out = pltpu.make_async_remote_copy(x_hbm.at[:, their_columns], xr.at[own_rows, their_columns], xsend, xrecv, partner, mesh_id)
    x_out.start()
    pass_on(True, 0)

    for s in range(4):
        wait_slot(2 + s)
        r = _dot(a[...], W[2 + s])
        for g in range(4):
            q[s, g * TOK : (g + 1) * TOK, :] = turn(r[:, g * HEAD : (g + 1) * HEAD], pl.ds(0, TOK))
        if s == 0:
            pass_on(True, 1)
        if s == 1:
            pass_on(False, 0)
            relay(0)
        if s == 2:
            pass_on(False, 1)
            relay(1)
            send(False, 2, (1,))
            send(False, 3, (1,))
    pass_on(True, 2)
    pass_on(False, 2, 0)
    pass_on(False, 3, 0)

    def attend(heads, js, first=False, beside=()):
        mask = None
        if first:
            mask = lax.broadcasted_iota(jnp.int32, (TOK, TOK), 0) <= lax.broadcasted_iota(jnp.int32, (TOK, TOK), 1)
        units = [(h, slice(g * TOK, (g + 1) * TOK)) for h in heads for g in range(4)]
        chunks, scores, weights, keeps = {}, {}, {}, {}

        def score(n):
            h, at = units[n]
            if h not in chunks:
                chunks[h] = []
                for j in js:
                    values = jnp.concatenate([kv[j, h, t, :, HEAD:] for t in range(2)], 0)
                    chunks[h].append((jnp.concatenate([kv[j, h, t, :, :HEAD] for t in range(2)], 0),
                                      jnp.concatenate([values.T, jnp.ones((8, TOK), BF16)], 0)))
            scores[n] = [_dot(keys, q[h, at, :], 1, 1) for keys, _ in chunks[h]]

        def weigh(n):
            h, at = units[n]
            some = scores.pop(n)
            if first:
                some = [jnp.where(mask, s, HIDDEN) for s in some]
            tops = [s.max(axis=0, keepdims=True) for s in some]
            top = functools.reduce(jnp.maximum, tops)
            if not first:
                old = top_s[h, :, at]
                top = jnp.maximum(old, top)
                keeps[n] = jnp.exp2((old - top) * E)
            top_s[h, :, at] = top
            weights[n] = [jnp.exp2((s - top) * E).astype(BF16) for s in some]

        def add(n):
            h, at = units[n]
            parts = [_dot(vt, p) for p, (_, vt) in zip(weights.pop(n), chunks[h])]
            total = functools.reduce(jnp.add, parts)
            acc[h, :, at] = total if first else acc[h, :, at] * keeps.pop(n) + total

        ahead = 4 if len(js) == 1 else 2
        steps = len(units) + ahead + 1
        for n in range(steps):
            if n < len(units):
                score(n)
            for piece in beside[len(beside) * n // steps : len(beside) * (n + 1) // steps]:
                piece()
            if 0 <= n - ahead < len(units):
                weigh(n - ahead)
            if 0 <= n - ahead - 1:
                add(n - ahead - 1)

    attend(range(4), [chip], True)
    pass_on(True, 3)

    def early(pair, beside=()):
        heads = (2 * pair, 2 * pair + 1)

        @pl.when(chip == 3)
        def _():
            if pair == 1:
                arrived(kv.at[1, pl.ds(2, 2), 1 - c], 10)
            arrived(kv.at[2, pl.ds(2 * pair, 2)], 2 + pair)
            attend(heads, [1, 2], beside=beside)

        @pl.when(chip == 2)
        def _():
            arrived(kv.at[0, pl.ds(2 * pair, 2), 0], 4 + pair)
            attend(heads, [0], beside=beside)

    def swap(pair):
        return pltpu.make_async_remote_copy(mine.at[pair], theirs.at[pair], asend, arecv.at[pair], partner, mesh_id)

    def late(pair):
        heads = (2 * pair, 2 * pair + 1)

        @pl.when(chip == 1)
        def _():
            arrived(kv.at[0, pl.ds(2 * pair, 2), 1], 4 + pair)

        @pl.when(chip == 2)
        def _():
            arrived(kv.at[1, pl.ds(2 * pair, 2)], 6 + pair)

        @pl.when(chip == 3)
        def _():
            arrived(kv.at[0, pl.ds(2 * pair, 2)], pair)

        @pl.when(chip > 0)
        def _():
            attend(heads, [jnp.where(chip == 2, 1, 0)])

        for i, h in enumerate(heads):
            for g in range(4):
                at = slice(g * TOK, (g + 1) * TOK)
                out = acc[h, :HEAD, at] * (1 / acc[h, HEAD : HEAD + 1, at])
                mine[pair, :, (4 * i + g) * HEAD : (4 * i + g + 1) * HEAD] = out.astype(BF16).T
        swap(pair).start()

    def blocks(slot, n):
        return W[slot, 1024 * n : 1024 * (n + 1), :]

    early(0)
    relay(2)
    late(0)
    relay(3)
    wait_slot(6)
    for n in range(NB):
        y[n] = _dot(mine[0], blocks(6, n))
    swap(0).wait_recv()
    wait_slot(7)

    def second_product(n, lo):
        y[n, :, lo : lo + TOK] += _dot(theirs[0], blocks(7, n)[:, lo : lo + TOK])

    pieces = [functools.partial(second_product, n, lo) for n in range(NB) for lo in range(0, N, TOK)]
    early(1, pieces)

    @pl.when(chip < 2)
    def _():
        for piece in pieces:
            piece()

    late(1)
    wait_slot(0)
    for n in range(NB):
        y[n] += _dot(mine[1], blocks(0, n))
    wait_slot(1)
    x_out.wait_recv()
    swap(1).wait_recv()

    def out_copy(n):
        at = pl.ds(pl.multiple_of(COLS * c + N * n, N), N)
        return pltpu.make_async_remote_copy(yo.at[n], y_out.at[:, at], ysend, yrecv, partner, mesh_id)

    def result(n, rows):
        at = pl.ds(pl.multiple_of(COLS * c + N * n, N), N)
        r = y[n, rows] + _dot(theirs[1, rows], blocks(1, n))
        return (xr[rows, at].astype(F32) + r).astype(BF16), at

    for group in ((0, 1, 2), (3, 4)):
        for n in group:
            yo[n], _ = result(n, their_rows)
        for n in group:
            out_copy(n).start()
    for n in range(NB):
        part, at = result(n, own_rows)
        y_out[:, at] = part

    def sent(units, sem):
        pltpu.make_async_copy(units, units, sem).wait()

    x_out.wait_send()
    sent(a.at[own_rows], nsend)
    sent(mine, asend)

    @pl.when(chip != 3)
    def _():
        sent(kv.at[0], ksend.at[0])

    @pl.when(chip == 0)
    def _():
        sent(kv.at[0], ksend.at[1])
        sent(kv.at[0, pl.ds(0, 2), 0], rsend)

    @pl.when(chip == 1)
    def _():
        sent(kv.at[0, pl.ds(0, 2), 0], ksend.at[1])

    @pl.when((chip == 1) | (chip == 2))
    def _():
        sent(kv.at[0, pl.ds(0, 4), 0], rsend)

    @pl.when(chip == 3)
    def _():
        sent(kv.at[0, pl.ds(0, 3)], rsend)

    sent(yo, ysend)
    sent(y_out.at[:, their_columns], yrecv)


def solution(mesh):
    turns = tables(4 * TOK)

    def step(x, gain, wq, wk, wv, wo):
        anywhere = pl.BlockSpec(memory_space=pl.ANY)
        dma = pltpu.SemaphoreType.DMA
        return pl.pallas_call(
            kernel,
            out_shape=pltpu.VMEM((OWN, D), BF16),
            in_specs=[anywhere] * 7,
            out_specs=pl.BlockSpec(memory_space=pltpu.VMEM),
            scratch_shapes=[
                pltpu.VMEM((SLOTS, D, N), BF16),
                pltpu.VMEM((TOK, D), BF16),
                pltpu.VMEM((TOK, D), BF16),
                pltpu.VMEM((D,), BF16),
                pltpu.VMEM((8, D), F32),
                pltpu.VMEM((TOK, HEAD), F32),
                pltpu.VMEM((TOK, HEAD), F32),
                pltpu.VMEM((4, 4 * TOK, HEAD), BF16),
                pltpu.VMEM((4, 4, 2, OWN, 2 * HEAD), BF16),
                pltpu.VMEM((4, HEAD + 8, 4 * TOK), F32),
                pltpu.VMEM((4, 1, 4 * TOK), F32),
                pltpu.VMEM((2, TOK, 1024), BF16),
                pltpu.VMEM((2, TOK, 1024), BF16),
                pltpu.VMEM((NB, TOK, N), F32),
                pltpu.VMEM((NB, OWN, N), BF16),
                dma((SLOTS - 2,)), dma((4,)), dma((PIECES,)), dma((2,)), dma, dma, dma, dma((2,)),
                dma((2,)), dma((11,)), dma, dma, dma((2,)), dma, dma,
            ],
            compiler_params=pltpu.CompilerParams(collective_id=0, has_side_effects=True, vmem_limit_bytes=62 * 2**20),
        )(x, gain, wq, wk, wv, wo, jnp.asarray(turns))

    tokens, whole = P(("dp", "sp"), None), P(None, None)
    return jax.shard_map(step, mesh=mesh, in_specs=(tokens, P(None), whole, whole, whole, whole), out_specs=tokens, check_vma=False)
```

```python
import functools

import jax
import jax.numpy as jnp
import numpy as np
from jax import lax
from jax.experimental import pallas as pl
from jax.experimental.pallas import tpu as pltpu
from jax.sharding import PartitionSpec as P

HEAD = 128
THETA = 10000
LOG2E = 1.4426950408889634
HIDDEN = -2e30
E = HEAD**-0.5 * LOG2E
F32, BF16 = jnp.float32, jnp.bfloat16

OWN = 128
TOK = 256
D = 5120
N = 512
COLS = D // 2
HALF = D // 2
NB = COLS // N
SLOTS = 8
PIECE = 64
PIECES = OWN // PIECE


def tables(rows):
    half = HEAD // 2
    power = np.float32(THETA) ** (-np.arange(half, dtype=np.float32) / np.float32(half))
    angle = np.arange(rows, dtype=np.float32)[:, None] * power.astype(np.float32)
    cos, sin = np.cos(angle.astype(np.float32)), np.sin(angle.astype(np.float32))
    return np.concatenate([cos, sin], 1).astype(np.float32)


def _dot(a, b, ca=1, cb=0):
    return lax.dot_general(a, b, (((ca,), (cb,)), ((), ())), preferred_element_type=F32)


def kernel(x_hbm, gain_hbm, wq, wk, wv, wo, turns_hbm, y_out,
           W, xr, a, gain, gain8, cos, sin, q, kv, acc, top_s, mine, theirs, y, yo,
           wsem, kvsem, xsem, tsem, xsend, xrecv, nsend, nrecv, ksend, krecv, rsend, asend, arecv, ysend, yrecv):
    me = lax.axis_index("sp")
    chip, c = me // 2, me % 2
    partner = {"sp": chip * 2 + (1 - c)}
    mesh_id = pl.DeviceIdType.MESH

    def there(chip_to):
        return {"sp": chip_to * 2 + c}

    def load_kv(h):
        at = pl.multiple_of((4 * c + h) * HEAD, HEAD)
        for part in range(2):
            rows = pl.ds(part * HALF, HALF)
            for n, w in enumerate((wk, wv)):
                to = W.at[h // 2, rows, pl.ds((h % 2) * 2 * HEAD + n * HEAD, HEAD)]
                sem = kvsem.at[part if h == 0 else min(h, 2) + 1]
                pltpu.make_async_copy(w.at[rows, pl.ds(at, HEAD)], to, sem).start(priority=1)

    def wait_kv(n):
        to = (W.at[0, pl.ds(0, HALF), pl.ds(0, 256)], W.at[0, pl.ds(HALF, HALF), pl.ds(0, 256)], W.at[0, :, pl.ds(256, 256)], W.at[1])[n]
        pltpu.make_async_copy(to, to, kvsem.at[n]).wait()

    def slot_sem(s):
        return wsem.at[s - 2] if s >= 2 else kvsem.at[s]

    def load_q(s):
        at = pl.multiple_of(2048 * c + N * s, N)
        pltpu.make_async_copy(wq.at[:, pl.ds(at, N)], W.at[2 + s], slot_sem(2 + s)).start(priority=1)

    def load_o(k, slot):
        side = c if k % 2 == 0 else 1 - c
        row = pl.multiple_of(2048 * side + 1024 * (k // 2), 1024)
        for n in range(NB):
            at = pl.multiple_of(COLS * c + N * n, N)
            to = W.at[slot, pl.ds(1024 * n, 1024), :]
            pltpu.make_async_copy(wo.at[pl.ds(row, 1024), pl.ds(at, N)], to, slot_sem(slot)).start(priority=1)

    def arrive(to, sem):
        pltpu.make_async_copy(to, to, sem).wait()

    def wait_slot(s):
        pltpu.make_async_copy(W.at[s], W.at[s], slot_sem(s)).wait()

    own_rows = pl.ds(pl.multiple_of(c * OWN, OWN), OWN)
    their_rows = pl.ds(pl.multiple_of((1 - c) * OWN, OWN), OWN)
    own_columns = pl.ds(pl.multiple_of(COLS * c, N), COLS)
    their_columns = pl.ds(pl.multiple_of(COLS * (1 - c), N), COLS)

    def rows_of(half, i):
        return pl.ds(pl.multiple_of(half * OWN + i * PIECE, PIECE), PIECE)

    x_in = [pltpu.make_async_copy(x_hbm.at[i * PIECE : (i + 1) * PIECE], xr.at[rows_of(c, i)], xsem.at[i]) for i in range(PIECES)]
    gain_in = pltpu.make_async_copy(gain_hbm, gain, tsem.at[0])
    gain_in.start()
    places = pl.ds(pl.multiple_of(chip * TOK, TOK), TOK)
    turns_in = pltpu.make_async_copy(turns_hbm.at[places], cos, tsem.at[1])
    turns_in.start()
    for piece in x_in:
        piece.start()
    for h in range(4):
        load_kv(h)
    for s in range(4):
        load_q(s)
    load_o(0, 6)
    load_o(1, 7)

    barrier = pltpu.get_barrier_semaphore()
    for peer in (partner, there(chip + 1 - 2 * (chip % 2)), there((chip + 2) % 4)):
        pl.semaphore_signal(barrier, inc=1, device_id=peer, device_id_type=mesh_id)
    pl.semaphore_wait(barrier, 3)

    gain_in.wait()
    gain8[...] = jnp.broadcast_to(gain[...].astype(F32)[None, :], (8, D))

    turns_in.wait()
    both = cos[...]
    other = pltpu.roll(both, 64, 1)
    low = lax.broadcasted_iota(jnp.int32, (TOK, HEAD), 1) < HEAD // 2
    cos[...] = jnp.where(low, both, other)
    sin[...] = jnp.where(low, -other, both)

    def norm_copy(i):
        part = a.at[rows_of(c, i), pl.ds(0, HALF)] if i < PIECES else a.at[own_rows, pl.ds(HALF, HALF)]
        return pltpu.make_async_remote_copy(part, part, nsend, nrecv.at[i // PIECES], partner, mesh_id)

    for i in range(PIECES):
        x_in[i].wait()
        first = c * OWN + i * PIECE
        groups = [pl.ds(pl.multiple_of(first + n * 16, 16), 16) for n in range(PIECE // 16)]
        scales = []
        for rows in groups:
            total = jnp.zeros((16, HEAD), F32)
            for at in range(0, D, HEAD):
                wide = xr[rows, at : at + HEAD].astype(F32)
                total += wide * wide
            scales.append(lax.rsqrt(jnp.sum(total, -1, keepdims=True) * (1 / D) + 1e-6))
        for at in range(0, D, HEAD):
            g = jnp.concatenate([gain8[:, at : at + HEAD]] * 2, 0)
            for rows, scale in zip(groups, scales):
                a[rows, at : at + HEAD] = (xr[rows, at : at + HEAD].astype(F32) * scale * g).astype(BF16)
        norm_copy(i).start()
    norm_copy(PIECES).start()

    def turn(t, rows):
        t = t.astype(BF16).astype(F32)
        return (t * cos[rows, :] + pltpu.roll(t, 64, 1) * sin[rows, :]).astype(BF16)

    def unit_copy(j, h, half, sem, chip_to, count):
        unit = kv.at[j, h, half]
        return pltpu.make_async_remote_copy(unit, unit, sem, krecv.at[count], there(chip_to), mesh_id)

    def arrived(units, count):
        pltpu.make_async_copy(units, units, krecv.at[count]).wait()

    def make_kv(rows, halves, heads, gates):
        lo = (heads[0] % 2) * 2 * HEAD
        columns = slice(lo, lo + len(heads) * 2 * HEAD)
        gates[0]()
        r = _dot(a[rows, :HALF], W[heads[0] // 2, :HALF, columns])
        gates[1]()
        r += _dot(a[rows, HALF:], W[heads[0] // 2, HALF:, columns])
        for i, h in enumerate(heads):
            keys = turn(r[:, i * 256 : i * 256 + HEAD], rows)
            values = r[:, i * 256 + HEAD : (i + 1) * 256].astype(BF16)
            for n, half in enumerate(halves):
                kv[chip, h, half, :, :HEAD] = keys[n * OWN : (n + 1) * OWN]
                kv[chip, h, half, :, HEAD:] = values[n * OWN : (n + 1) * OWN]

    def send(own, h, chips=(0, 1, 2)):
        half = c if own else 1 - c
        if 0 in chips:
            @pl.when(chip == 0)
            def _():
                for n in range(2):
                    unit_copy(chip, h, half, ksend.at[n], n + 1, jnp.where(half == n, h, 4 + h // 2)).start()

        if 1 in chips:
            @pl.when((chip == 1) | (chip == 2))
            def _():
                count = jnp.where(chip == 2, 2 + h // 2, 4 + h if own else min(8 + h, 10))
                unit_copy(chip, h, half, ksend.at[0], 3, count).start()

    def pass_on(own, h, by=3):
        half = c if own else 1 - c

        @pl.when(chip == by)
        def _():
            arrived(kv.at[1, h, half], h - 2 if by == 0 else 4 + h if own else 8 + h)
            unit_copy(1, h, half, rsend, 2, 6 + h // 2).start()

    def relay(h):
        for p in (1, 2):
            @pl.when(chip == p)
            def _():
                arrived(kv.at[0, h, p - 1], h)
                unit_copy(0, h, p - 1, rsend, 3, h // 2).start()

    def gate(*waits):
        def run():
            for wait in waits:
                wait()
        return run

    make_kv(own_rows, (c,), (0,), (gate(functools.partial(wait_kv, 0)), gate(functools.partial(wait_kv, 1))))
    send(True, 0)
    make_kv(own_rows, (c,), (1,), (gate(functools.partial(wait_kv, 2)), gate()))
    send(True, 1)
    def theirs_here(n):
        part = a.at[their_rows, pl.ds(n * HALF, HALF)]
        pltpu.make_async_copy(part, part, nrecv.at[n]).wait()

    halves = gate(functools.partial(theirs_here, 0)), gate(functools.partial(theirs_here, 1))
    make_kv(their_rows, (1 - c,), (0, 1), halves)
    send(False, 0)
    send(False, 1)
    make_kv(pl.ds(0, TOK), (0, 1), (2, 3), (gate(functools.partial(wait_kv, 3)), gate()))
    for h in (2, 3):
        send(True, h)
    for h in (2, 3):
        send(False, h, (0,))

        @pl.when(chip == 1)
        def _():
            unit_copy(chip, h, 1 - c, ksend.at[1], 0, h - 2).start()

    load_o(2, 0)
    load_o(3, 1)
    x_out = pltpu.make_async_remote_copy(x_hbm.at[:, their_columns], xr.at[own_rows, their_columns], xsend, xrecv, partner, mesh_id)
    x_out.start()
    pass_on(True, 0)

    def put_q(s, r):
        for g in range(4):
            q[s, g * TOK : (g + 1) * TOK, :] = turn(r[:, g * HEAD : (g + 1) * HEAD], pl.ds(0, TOK))

    for s in range(4):
        wait_slot(2 + s)
        r = _dot(a[...], W[2 + s])
        if s:
            put_q(s - 1, before)
        before = r
        if s == 0:
            pass_on(True, 1)
        if s == 1:
            pass_on(False, 0)
            relay(0)
        if s == 2:
            pass_on(False, 1)
            relay(1)
            send(False, 2, (1,))
            send(False, 3, (1,))

    def attend(heads, js, first=False, beside=()):
        mask = None
        if first:
            mask = lax.broadcasted_iota(jnp.int32, (TOK, TOK), 0) <= lax.broadcasted_iota(jnp.int32, (TOK, TOK), 1)
        units = [(h, slice(g * TOK, (g + 1) * TOK)) for h in heads for g in range(4)]
        chunks, scores, weights, keeps = {}, {}, {}, {}

        def score(n):
            h, at = units[n]
            if h not in chunks:
                chunks[h] = []
                for j in js:
                    values = jnp.concatenate([kv[j, h, t, :, HEAD:] for t in range(2)], 0)
                    chunks[h].append((jnp.concatenate([kv[j, h, t, :, :HEAD] for t in range(2)], 0),
                                      jnp.concatenate([values.T, jnp.ones((8, TOK), BF16)], 0)))
            scores[n] = [_dot(keys, q[h, at, :], 1, 1) for keys, _ in chunks[h]]

        def weigh(n):
            h, at = units[n]
            some = scores.pop(n)
            if first:
                some = [jnp.where(mask, s, HIDDEN) for s in some]
            tops = [s.max(axis=0, keepdims=True) for s in some]
            top = functools.reduce(jnp.maximum, tops)
            if not first:
                old = top_s[h, :, at]
                top = jnp.maximum(old, top)
                keeps[n] = jnp.exp2((old - top) * E)
            top_s[h, :, at] = top
            weights[n] = [jnp.exp2((s - top) * E).astype(BF16) for s in some]

        def add(n):
            h, at = units[n]
            parts = [_dot(vt, p) for p, (_, vt) in zip(weights.pop(n), chunks[h])]
            total = functools.reduce(jnp.add, parts)
            acc[h, :, at] = total if first else acc[h, :, at] * keeps.pop(n) + total

        ahead = 4 if len(js) == 1 else 2
        steps = len(units) + ahead + 1
        for n in range(steps):
            if n < len(units):
                score(n)
            for piece in beside[len(beside) * n // steps : len(beside) * (n + 1) // steps]:
                piece()
            if 0 <= n - ahead < len(units):
                weigh(n - ahead)
            if 0 <= n - ahead - 1:
                add(n - ahead - 1)

    put_q(3, before)
    attend(range(4), [chip], True)
    pass_on(True, 2)
    pass_on(True, 3)
    pass_on(False, 2, 0)
    pass_on(False, 3, 0)

    def early(pair, beside=()):
        heads = (2 * pair, 2 * pair + 1)

        @pl.when(chip == 3)
        def _():
            if pair == 1:
                arrived(kv.at[1, pl.ds(2, 2), 1 - c], 10)
            arrived(kv.at[2, pl.ds(2 * pair, 2)], 2 + pair)
            attend(heads, [1, 2], beside=beside)

    def swap(pair, rows, sem):
        return pltpu.make_async_remote_copy(mine.at[pair, rows], theirs.at[pair, rows], asend, arecv.at[sem], partner, mesh_id)

    def late(pair):
        heads = (2 * pair, 2 * pair + 1)

        def chunk(j, _):
            @pl.when(chip == 1)
            def _():
                arrived(kv.at[0, pl.ds(2 * pair, 2), 1], 4 + pair)

            @pl.when((chip == 2) & (j == 0))
            def _():
                arrived(kv.at[0, pl.ds(2 * pair, 2), 0], 4 + pair)

            @pl.when((chip == 2) & (j == 1))
            def _():
                arrived(kv.at[1, pl.ds(2 * pair, 2)], 6 + pair)

            @pl.when(chip == 3)
            def _():
                arrived(kv.at[0, pl.ds(2 * pair, 2)], pair)

            attend(heads, [j])

        lax.fori_loop(0, jnp.where(chip == 2, 2, jnp.minimum(chip, 1)), chunk, None)

        def finish(first, rows):
            for i, h in enumerate(heads):
                for g in range(4):
                    at = pl.ds(pl.multiple_of(g * TOK + first, OWN), rows.size)
                    out = acc[h, :HEAD, at] * (1 / acc[h, HEAD : HEAD + 1, at])
                    mine[pair, rows, (4 * i + g) * HEAD : (4 * i + g + 1) * HEAD] = out.astype(BF16).T

        if pair == 0:
            finish(0, pl.ds(0, TOK))
            swap(0, pl.ds(0, TOK), 0).start()
        else:
            finish(c * OWN, own_rows)
            swap(1, own_rows, 1).start()
            finish((1 - c) * OWN, their_rows)
            swap(1, their_rows, 2).start()

    def blocks(slot, n):
        return W[slot, 1024 * n : 1024 * (n + 1), :]

    early(0)
    relay(2)
    late(0)
    relay(3)
    wait_slot(6)
    for n in range(NB):
        y[n] = _dot(mine[0], blocks(6, n))
    arrive(theirs.at[0], arecv.at[0])
    wait_slot(7)

    def second_product(n, lo):
        y[n, :, lo : lo + TOK] += _dot(theirs[0], blocks(7, n)[:, lo : lo + TOK])

    pieces = [functools.partial(second_product, n, lo) for n in range(NB) for lo in range(0, N, TOK)]
    early(1, pieces)

    @pl.when(chip < 3)
    def _():
        for piece in pieces:
            piece()

    late(1)
    wait_slot(0)

    def third(n, rows):
        return _dot(mine[1, rows], blocks(0, n))

    for n in range(NB):
        y[n, their_rows] += third(n, their_rows)
    for n in range(4):
        y[n, own_rows] += third(n, own_rows)
    wait_slot(1)
    x_out.wait_recv()
    arrive(theirs.at[1, their_rows], arecv.at[1])

    def out_copy(n):
        at = pl.ds(pl.multiple_of(COLS * c + N * n, N), N)
        return pltpu.make_async_remote_copy(yo.at[n], y_out.at[:, at], ysend, yrecv, partner, mesh_id)

    def result(n, rows, more=False):
        at = pl.ds(pl.multiple_of(COLS * c + N * n, N), N)
        r = _dot(theirs[1, rows], blocks(1, n))
        r = y[n, rows] + (third(n, rows) + r if more else r)
        return (xr[rows, at].astype(F32) + r).astype(BF16), at

    for group in ((0, 1), (2, 3), (4,)):
        for n in group:
            yo[n], _ = result(n, their_rows)
        for n in group:
            out_copy(n).start()
    arrive(theirs.at[1, own_rows], arecv.at[2])
    for n in range(NB):
        part, at = result(n, own_rows, n >= 4)
        y_out[:, at] = part

    x_out.wait_send()
    arrive(a.at[own_rows], nsend)
    arrive(mine, asend)

    @pl.when(chip != 3)
    def _():
        arrive(kv.at[0], ksend.at[0])

    @pl.when(chip == 0)
    def _():
        arrive(kv.at[0], ksend.at[1])
        arrive(kv.at[0, pl.ds(0, 2), 0], rsend)

    @pl.when(chip == 1)
    def _():
        arrive(kv.at[0, pl.ds(0, 2), 0], ksend.at[1])

    @pl.when((chip == 1) | (chip == 2))
    def _():
        arrive(kv.at[0, pl.ds(0, 4), 0], rsend)

    @pl.when(chip == 3)
    def _():
        arrive(kv.at[0, pl.ds(0, 3)], rsend)

    arrive(yo, ysend)
    arrive(y_out.at[:, their_columns], yrecv)


def solution(mesh):
    turns = tables(4 * TOK)

    def step(x, gain, wq, wk, wv, wo):
        anywhere = pl.BlockSpec(memory_space=pl.ANY)
        dma = pltpu.SemaphoreType.DMA
        return pl.pallas_call(
            kernel,
            out_shape=pltpu.VMEM((OWN, D), BF16),
            in_specs=[anywhere] * 7,
            out_specs=pl.BlockSpec(memory_space=pltpu.VMEM),
            scratch_shapes=[
                pltpu.VMEM((SLOTS, D, N), BF16),
                pltpu.VMEM((TOK, D), BF16),
                pltpu.VMEM((TOK, D), BF16),
                pltpu.VMEM((D,), BF16),
                pltpu.VMEM((8, D), F32),
                pltpu.VMEM((TOK, HEAD), F32),
                pltpu.VMEM((TOK, HEAD), F32),
                pltpu.VMEM((4, 4 * TOK, HEAD), BF16),
                pltpu.VMEM((4, 4, 2, OWN, 2 * HEAD), BF16),
                pltpu.VMEM((4, HEAD + 8, 4 * TOK), F32),
                pltpu.VMEM((4, 1, 4 * TOK), F32),
                pltpu.VMEM((2, TOK, 1024), BF16),
                pltpu.VMEM((2, TOK, 1024), BF16),
                pltpu.VMEM((NB, TOK, N), F32),
                pltpu.VMEM((NB, OWN, N), BF16),
                dma((SLOTS - 2,)), dma((4,)), dma((PIECES,)), dma((2,)), dma, dma, dma, dma((2,)),
                dma((2,)), dma((11,)), dma, dma, dma((3,)), dma, dma,
            ],
            compiler_params=pltpu.CompilerParams(collective_id=0, has_side_effects=True, vmem_limit_bytes=62 * 2**20),
        )(x, gain, wq, wk, wv, wo, jnp.asarray(turns))

    tokens, whole = P(("dp", "sp"), None), P(None, None)
    return jax.shard_map(step, mesh=mesh, in_specs=(tokens, P(None), whole, whole, whole, whole), out_specs=tokens, check_vma=False)
```

```python
import functools

import jax
import jax.numpy as jnp
import numpy as np
from jax import lax
from jax.experimental import pallas as pl
from jax.experimental.pallas import tpu as pltpu
from jax.sharding import PartitionSpec as P

HEAD = 128
THETA = 10000
LOG2E = 1.4426950408889634
HIDDEN = -2e30
E = HEAD**-0.5 * LOG2E
F32, BF16 = jnp.float32, jnp.bfloat16

OWN = 128
TOK = 256
D = 5120
N = 512
COLS = D // 2
HALF = D // 2
NB = COLS // N
SLOTS = 8
PIECE = 64
PIECES = OWN // PIECE


def tables(rows):
    half = HEAD // 2
    power = np.float32(THETA) ** (-np.arange(half, dtype=np.float32) / np.float32(half))
    angle = np.arange(rows, dtype=np.float32)[:, None] * power.astype(np.float32)
    cos, sin = np.cos(angle.astype(np.float32)), np.sin(angle.astype(np.float32))
    return np.concatenate([cos, sin], 1).astype(np.float32)


def _dot(a, b, ca=1, cb=0):
    return lax.dot_general(a, b, (((ca,), (cb,)), ((), ())), preferred_element_type=F32)


def kernel(x_hbm, gain_hbm, wq, wk, wv, wo, turns_hbm, y_out,
           W, xr, a, gain, gain8, cos, sin, q, kv, acc, top_s, mine, theirs, y, yo,
           wsem, kvsem, xsem, tsem, xsend, xrecv, nsend, nrecv, ksend, krecv, rsend, asend, arecv, ysend, yrecv):
    me = lax.axis_index("sp")
    chip, c = me // 2, me % 2
    partner = {"sp": chip * 2 + (1 - c)}
    mesh_id = pl.DeviceIdType.MESH

    def there(chip_to):
        return {"sp": chip_to * 2 + c}

    def load_kv(h):
        at = pl.multiple_of((4 * c + h) * HEAD, HEAD)
        for part in range(2):
            rows = pl.ds(part * HALF, HALF)
            for n, w in enumerate((wk, wv)):
                to = W.at[h // 2, rows, pl.ds((h % 2) * 2 * HEAD + n * HEAD, HEAD)]
                sem = kvsem.at[part if h == 0 else min(h, 2) + 1]
                pltpu.make_async_copy(w.at[rows, pl.ds(at, HEAD)], to, sem).start(priority=1)

    def wait_kv(n):
        to = (W.at[0, pl.ds(0, HALF), pl.ds(0, 256)], W.at[0, pl.ds(HALF, HALF), pl.ds(0, 256)], W.at[0, :, pl.ds(256, 256)], W.at[1])[n]
        pltpu.make_async_copy(to, to, kvsem.at[n]).wait()

    def slot_sem(s):
        return wsem.at[s - 2] if s >= 2 else kvsem.at[s]

    def load_q(s):
        at = pl.multiple_of(2048 * c + N * s, N)
        pltpu.make_async_copy(wq.at[:, pl.ds(at, N)], W.at[2 + s], slot_sem(2 + s)).start(priority=1)

    def load_o(k, slot):
        side = c if k % 2 == 0 else 1 - c
        row = pl.multiple_of(2048 * side + 1024 * (k // 2), 1024)
        for n in range(NB):
            at = pl.multiple_of(COLS * c + N * n, N)
            to = W.at[slot, pl.ds(1024 * n, 1024), :]
            pltpu.make_async_copy(wo.at[pl.ds(row, 1024), pl.ds(at, N)], to, slot_sem(slot)).start(priority=1)

    def arrive(to, sem):
        pltpu.make_async_copy(to, to, sem).wait()

    def wait_slot(s):
        pltpu.make_async_copy(W.at[s], W.at[s], slot_sem(s)).wait()

    own_rows = pl.ds(pl.multiple_of(c * OWN, OWN), OWN)
    their_rows = pl.ds(pl.multiple_of((1 - c) * OWN, OWN), OWN)
    own_columns = pl.ds(pl.multiple_of(COLS * c, N), COLS)
    their_columns = pl.ds(pl.multiple_of(COLS * (1 - c), N), COLS)

    def rows_of(half, i):
        return pl.ds(pl.multiple_of(half * OWN + i * PIECE, PIECE), PIECE)

    x_in = [pltpu.make_async_copy(x_hbm.at[i * PIECE : (i + 1) * PIECE], xr.at[rows_of(c, i)], xsem.at[i]) for i in range(PIECES)]
    gain_in = pltpu.make_async_copy(gain_hbm, gain, tsem.at[0])
    gain_in.start()
    for piece in x_in:
        piece.start()
    places = pl.ds(pl.multiple_of(chip * TOK, TOK), TOK)
    turns_in = pltpu.make_async_copy(turns_hbm.at[places], cos, tsem.at[1])
    turns_in.start()
    for h in range(4):
        load_kv(h)
    for s in range(4):
        load_q(s)
    load_o(0, 6)
    load_o(1, 7)

    barrier = pltpu.get_barrier_semaphore()
    for peer in (partner, there(chip + 1 - 2 * (chip % 2)), there((chip + 2) % 4)):
        pl.semaphore_signal(barrier, inc=1, device_id=peer, device_id_type=mesh_id)
    pl.semaphore_wait(barrier, 3)

    gain_in.wait()
    gain8[...] = jnp.broadcast_to(gain[...].astype(F32)[None, :], (8, D))

    def norm_copy(i):
        part = a.at[rows_of(c, i), pl.ds(0, HALF)] if i < PIECES else a.at[own_rows, pl.ds(HALF, HALF)]
        return pltpu.make_async_remote_copy(part, part, nsend, nrecv.at[i // PIECES], partner, mesh_id)

    for i in range(PIECES):
        x_in[i].wait()
        first = c * OWN + i * PIECE
        groups = [pl.ds(pl.multiple_of(first + n * 16, 16), 16) for n in range(PIECE // 16)]
        scales = []
        for rows in groups:
            total = jnp.zeros((16, HEAD), F32)
            for at in range(0, D, HEAD):
                wide = xr[rows, at : at + HEAD].astype(F32)
                total += wide * wide
            scales.append(lax.rsqrt(jnp.sum(total, -1, keepdims=True) * (1 / D) + 1e-6))
        for at in range(0, D, HEAD):
            g = jnp.concatenate([gain8[:, at : at + HEAD]] * 2, 0)
            for rows, scale in zip(groups, scales):
                a[rows, at : at + HEAD] = (xr[rows, at : at + HEAD].astype(F32) * scale * g).astype(BF16)
        norm_copy(i).start()
    norm_copy(PIECES).start()

    turns_in.wait()
    both = cos[...]
    other = pltpu.roll(both, 64, 1)
    low = lax.broadcasted_iota(jnp.int32, (TOK, HEAD), 1) < HEAD // 2
    cos[...] = jnp.where(low, both, other)
    sin[...] = jnp.where(low, -other, both)

    def turn(t, rows):
        t = t.astype(BF16).astype(F32)
        return (t * cos[rows, :] + pltpu.roll(t, 64, 1) * sin[rows, :]).astype(BF16)

    def unit_copy(j, h, half, sem, chip_to, count):
        unit = kv.at[j, h, half]
        return pltpu.make_async_remote_copy(unit, unit, sem, krecv.at[count], there(chip_to), mesh_id)

    def arrived(units, count):
        pltpu.make_async_copy(units, units, krecv.at[count]).wait()

    def make_kv(rows, halves, heads, gates):
        lo = (heads[0] % 2) * 2 * HEAD
        columns = slice(lo, lo + len(heads) * 2 * HEAD)
        gates[0]()
        r = _dot(a[rows, :HALF], W[heads[0] // 2, :HALF, columns])
        gates[1]()
        r += _dot(a[rows, HALF:], W[heads[0] // 2, HALF:, columns])
        for i, h in enumerate(heads):
            keys = turn(r[:, i * 256 : i * 256 + HEAD], rows)
            values = r[:, i * 256 + HEAD : (i + 1) * 256].astype(BF16)
            for n, half in enumerate(halves):
                kv[chip, h, half, :, :HEAD] = keys[n * OWN : (n + 1) * OWN]
                kv[chip, h, half, :, HEAD:] = values[n * OWN : (n + 1) * OWN]

    def send(own, h, chips=(0, 1, 2)):
        half = c if own else 1 - c
        if 0 in chips:
            @pl.when(chip == 0)
            def _():
                for n in range(2):
                    unit_copy(chip, h, half, ksend.at[n], n + 1, jnp.where(half == n, h, 4 + h // 2)).start()

        if 1 in chips:
            @pl.when((chip == 1) | (chip == 2))
            def _():
                count = jnp.where(chip == 2, 2 + h // 2, 4 + h if own else min(8 + h, 10))
                unit_copy(chip, h, half, ksend.at[0], 3, count).start()

    def pass_on(own, h, by=3):
        half = c if own else 1 - c

        @pl.when(chip == by)
        def _():
            arrived(kv.at[1, h, half], h - 2 if by == 0 else 4 + h if own else 8 + h)
            unit_copy(1, h, half, rsend, 2, 6 + h // 2).start()

    def relay(h):
        for p in (1, 2):
            @pl.when(chip == p)
            def _():
                arrived(kv.at[0, h, p - 1], h)
                unit_copy(0, h, p - 1, rsend, 3, h // 2).start()

    def gate(*waits):
        def run():
            for wait in waits:
                wait()
        return run

    make_kv(own_rows, (c,), (0,), (gate(functools.partial(wait_kv, 0)), gate(functools.partial(wait_kv, 1))))
    send(True, 0)
    make_kv(own_rows, (c,), (1,), (gate(functools.partial(wait_kv, 2)), gate()))
    send(True, 1)
    def theirs_here(n):
        part = a.at[their_rows, pl.ds(n * HALF, HALF)]
        pltpu.make_async_copy(part, part, nrecv.at[n]).wait()

    halves = gate(functools.partial(theirs_here, 0)), gate(functools.partial(theirs_here, 1))
    make_kv(their_rows, (1 - c,), (0, 1), halves)
    send(False, 0)
    send(False, 1)
    make_kv(pl.ds(0, TOK), (0, 1), (2, 3), (gate(functools.partial(wait_kv, 3)), gate()))
    for h in (2, 3):
        send(True, h)
    for h in (2, 3):
        send(False, h, (0,))

        @pl.when(chip == 1)
        def _():
            unit_copy(chip, h, 1 - c, ksend.at[1], 0, h - 2).start()

    load_o(2, 0)
    load_o(3, 1)
    x_out = pltpu.make_async_remote_copy(x_hbm.at[:, their_columns], xr.at[own_rows, their_columns], xsend, xrecv, partner, mesh_id)
    x_out.start()
    pass_on(True, 0)

    def put_q(s, r):
        for g in range(4):
            q[s, g * TOK : (g + 1) * TOK, :] = turn(r[:, g * HEAD : (g + 1) * HEAD], pl.ds(0, TOK))

    for s in range(4):
        wait_slot(2 + s)
        r = _dot(a[...], W[2 + s])
        if s:
            put_q(s - 1, before)
        before = r
        if s == 0:
            pass_on(True, 1)
        if s == 1:
            pass_on(False, 0)
            relay(0)
        if s == 2:
            pass_on(False, 1)
            relay(1)
            send(False, 2, (1,))
            send(False, 3, (1,))

    def attend(heads, js, first=False, beside=()):
        mask = None
        if first:
            mask = lax.broadcasted_iota(jnp.int32, (TOK, TOK), 0) <= lax.broadcasted_iota(jnp.int32, (TOK, TOK), 1)
        units = [(h, slice(g * TOK, (g + 1) * TOK)) for h in heads for g in range(4)]
        chunks, scores, weights, keeps = {}, {}, {}, {}

        def score(n):
            h, at = units[n]
            if h not in chunks:
                chunks[h] = []
                for j in js:
                    values = jnp.concatenate([kv[j, h, t, :, HEAD:] for t in range(2)], 0)
                    chunks[h].append((jnp.concatenate([kv[j, h, t, :, :HEAD] for t in range(2)], 0),
                                      jnp.concatenate([values.T, jnp.ones((8, TOK), BF16)], 0)))
            scores[n] = [_dot(keys, q[h, at, :], 1, 1) for keys, _ in chunks[h]]

        def weigh(n):
            h, at = units[n]
            some = scores.pop(n)
            if first:
                some = [jnp.where(mask, s, HIDDEN) for s in some]
            tops = [s.max(axis=0, keepdims=True) for s in some]
            top = functools.reduce(jnp.maximum, tops)
            if not first:
                old = top_s[h, :, at]
                top = jnp.maximum(old, top)
                keeps[n] = jnp.exp2((old - top) * E)
            top_s[h, :, at] = top
            weights[n] = [jnp.exp2((s - top) * E).astype(BF16) for s in some]

        def add(n):
            h, at = units[n]
            parts = [_dot(vt, p) for p, (_, vt) in zip(weights.pop(n), chunks[h])]
            total = functools.reduce(jnp.add, parts)
            acc[h, :, at] = total if first else acc[h, :, at] * keeps.pop(n) + total

        ahead = 4 if len(js) == 1 else 2
        steps = len(units) + ahead + 1
        for n in range(steps):
            if n < len(units):
                score(n)
            for piece in beside[len(beside) * n // steps : len(beside) * (n + 1) // steps]:
                piece()
            if 0 <= n - ahead < len(units):
                weigh(n - ahead)
            if 0 <= n - ahead - 1:
                add(n - ahead - 1)

    put_q(3, before)
    attend(range(4), [chip], True)
    pass_on(True, 2)
    pass_on(True, 3)
    pass_on(False, 2, 0)
    pass_on(False, 3, 0)

    def early(pair, beside=()):
        heads = (2 * pair, 2 * pair + 1)

        @pl.when(chip == 3)
        def _():
            if pair == 1:
                arrived(kv.at[1, pl.ds(2, 2), 1 - c], 10)
            arrived(kv.at[2, pl.ds(2 * pair, 2)], 2 + pair)
            attend(heads, [1, 2], beside=beside)

    def swap(pair, rows, sem):
        return pltpu.make_async_remote_copy(mine.at[pair, rows], theirs.at[pair, rows], asend, arecv.at[sem], partner, mesh_id)

    def late(pair):
        heads = (2 * pair, 2 * pair + 1)

        def chunk(j, _):
            @pl.when(chip == 1)
            def _():
                arrived(kv.at[0, pl.ds(2 * pair, 2), 1], 4 + pair)

            @pl.when((chip == 2) & (j == 0))
            def _():
                arrived(kv.at[0, pl.ds(2 * pair, 2), 0], 4 + pair)

            @pl.when((chip == 2) & (j == 1))
            def _():
                arrived(kv.at[1, pl.ds(2 * pair, 2)], 6 + pair)

            @pl.when(chip == 3)
            def _():
                arrived(kv.at[0, pl.ds(2 * pair, 2)], pair)

            attend(heads, [j])

        lax.fori_loop(0, jnp.where(chip == 2, 2, jnp.minimum(chip, 1)), chunk, None)

        def finish(first, rows):
            for i, h in enumerate(heads):
                for g in range(4):
                    at = pl.ds(pl.multiple_of(g * TOK + first, OWN), rows.size)
                    out = acc[h, :HEAD, at] * (1 / acc[h, HEAD : HEAD + 1, at])
                    mine[pair, rows, (4 * i + g) * HEAD : (4 * i + g + 1) * HEAD] = out.astype(BF16).T

        if pair == 0:
            finish(0, pl.ds(0, TOK))
            swap(0, pl.ds(0, TOK), 0).start()
        else:
            finish(c * OWN, own_rows)
            swap(1, own_rows, 1).start()
            finish((1 - c) * OWN, their_rows)
            swap(1, their_rows, 2).start()

    def blocks(slot, n):
        return W[slot, 1024 * n : 1024 * (n + 1), :]

    early(0)
    relay(2)
    late(0)
    relay(3)
    wait_slot(6)
    for n in range(NB):
        y[n] = _dot(mine[0], blocks(6, n))
    arrive(theirs.at[0], arecv.at[0])
    wait_slot(7)

    def second_product(n, lo):
        y[n, :, lo : lo + TOK] += _dot(theirs[0], blocks(7, n)[:, lo : lo + TOK])

    pieces = [functools.partial(second_product, n, lo) for n in range(NB) for lo in range(0, N, TOK)]
    early(1, pieces)

    @pl.when(chip < 3)
    def _():
        for piece in pieces:
            piece()

    late(1)
    wait_slot(0)

    def third(n, rows):
        return _dot(mine[1, rows], blocks(0, n))

    for n in range(NB):
        y[n, their_rows] += third(n, their_rows)
    for n in range(4):
        y[n, own_rows] += third(n, own_rows)
    wait_slot(1)
    x_out.wait_recv()
    arrive(theirs.at[1, their_rows], arecv.at[1])

    def out_copy(n):
        at = pl.ds(pl.multiple_of(COLS * c + N * n, N), N)
        return pltpu.make_async_remote_copy(yo.at[n], y_out.at[:, at], ysend, yrecv, partner, mesh_id)

    def result(n, rows, more=False):
        at = pl.ds(pl.multiple_of(COLS * c + N * n, N), N)
        r = _dot(theirs[1, rows], blocks(1, n))
        r = y[n, rows] + (third(n, rows) + r if more else r)
        return (xr[rows, at].astype(F32) + r).astype(BF16), at

    for group in ((0, 1), (2, 3), (4,)):
        for n in group:
            yo[n], _ = result(n, their_rows)
        for n in group:
            out_copy(n).start()
    arrive(theirs.at[1, own_rows], arecv.at[2])
    for n in range(NB):
        part, at = result(n, own_rows, n >= 4)
        y_out[:, at] = part

    x_out.wait_send()
    arrive(a.at[own_rows], nsend)
    arrive(mine, asend)

    @pl.when(chip != 3)
    def _():
        arrive(kv.at[0], ksend.at[0])

    @pl.when(chip == 0)
    def _():
        arrive(kv.at[0], ksend.at[1])
        arrive(kv.at[0, pl.ds(0, 2), 0], rsend)

    @pl.when(chip == 1)
    def _():
        arrive(kv.at[0, pl.ds(0, 2), 0], ksend.at[1])

    @pl.when((chip == 1) | (chip == 2))
    def _():
        arrive(kv.at[0, pl.ds(0, 4), 0], rsend)

    @pl.when(chip == 3)
    def _():
        arrive(kv.at[0, pl.ds(0, 3)], rsend)

    arrive(yo, ysend)
    arrive(y_out.at[:, their_columns], yrecv)


def solution(mesh):
    turns = tables(4 * TOK)

    def step(x, gain, wq, wk, wv, wo):
        anywhere = pl.BlockSpec(memory_space=pl.ANY)
        dma = pltpu.SemaphoreType.DMA
        return pl.pallas_call(
            kernel,
            out_shape=pltpu.VMEM((OWN, D), BF16),
            in_specs=[anywhere] * 7,
            out_specs=pl.BlockSpec(memory_space=pltpu.VMEM),
            scratch_shapes=[
                pltpu.VMEM((SLOTS, D, N), BF16),
                pltpu.VMEM((TOK, D), BF16),
                pltpu.VMEM((TOK, D), BF16),
                pltpu.VMEM((D,), BF16),
                pltpu.VMEM((8, D), F32),
                pltpu.VMEM((TOK, HEAD), F32),
                pltpu.VMEM((TOK, HEAD), F32),
                pltpu.VMEM((4, 4 * TOK, HEAD), BF16),
                pltpu.VMEM((4, 4, 2, OWN, 2 * HEAD), BF16),
                pltpu.VMEM((4, HEAD + 8, 4 * TOK), F32),
                pltpu.VMEM((4, 1, 4 * TOK), F32),
                pltpu.VMEM((2, TOK, 1024), BF16),
                pltpu.VMEM((2, TOK, 1024), BF16),
                pltpu.VMEM((NB, TOK, N), F32),
                pltpu.VMEM((NB, OWN, N), BF16),
                dma((SLOTS - 2,)), dma((4,)), dma((PIECES,)), dma((2,)), dma, dma, dma, dma((2,)),
                dma((2,)), dma((11,)), dma, dma, dma((3,)), dma, dma,
            ],
            compiler_params=pltpu.CompilerParams(collective_id=0, has_side_effects=True, vmem_limit_bytes=62 * 2**20),
        )(x, gain, wq, wk, wv, wo, jnp.asarray(turns))

    tokens, whole = P(("dp", "sp"), None), P(None, None)
    return jax.shard_map(step, mesh=mesh, in_specs=(tokens, P(None), whole, whole, whole, whole), out_specs=tokens, check_vma=False)
```

```python
import functools

import jax
import jax.numpy as jnp
import numpy as np
from jax import lax
from jax.experimental import pallas as pl
from jax.experimental.pallas import tpu as pltpu
from jax.sharding import PartitionSpec as P

HEAD = 128
THETA = 10000
LOG2E = 1.4426950408889634
HIDDEN = -2e30
E = HEAD**-0.5 * LOG2E
F32, BF16 = jnp.float32, jnp.bfloat16

OWN = 128
TOK = 256
D = 5120
N = 512
COLS = D // 2
HALF = D // 2
NB = COLS // N
SLOTS = 8
PIECE = 64
PIECES = OWN // PIECE


def tables(rows):
    half = HEAD // 2
    power = np.float32(THETA) ** (-np.arange(half, dtype=np.float32) / np.float32(half))
    angle = np.arange(rows, dtype=np.float32)[:, None] * power.astype(np.float32)
    cos, sin = np.cos(angle.astype(np.float32)), np.sin(angle.astype(np.float32))
    return np.concatenate([cos, sin], 1).astype(np.float32)


def _dot(a, b, ca=1, cb=0):
    return lax.dot_general(a, b, (((ca,), (cb,)), ((), ())), preferred_element_type=F32)


def kernel(x_hbm, gain_hbm, wq, wk, wv, wo, turns_hbm, y_out,
           W, xr, a, gain, gain8, cos, sin, q, kv, acc, top_s, mine, theirs, y, yo,
           wsem, kvsem, xsem, tsem, xsend, xrecv, nsend, nrecv, ksend, krecv, rsend, asend, arecv, ysend, yrecv):
    me = lax.axis_index("sp")
    chip, c = me // 2, me % 2
    partner = {"sp": chip * 2 + (1 - c)}
    mesh_id = pl.DeviceIdType.MESH

    def there(chip_to):
        return {"sp": chip_to * 2 + c}

    def load_kv(h):
        at = pl.multiple_of((4 * c + h) * HEAD, HEAD)
        for part in range(2):
            rows = pl.ds(part * HALF, HALF)
            for n, w in enumerate((wk, wv)):
                to = W.at[h // 2, rows, pl.ds((h % 2) * 2 * HEAD + n * HEAD, HEAD)]
                sem = kvsem.at[part if h == 0 else min(h, 2) + 1]
                pltpu.make_async_copy(w.at[rows, pl.ds(at, HEAD)], to, sem).start(priority=1)

    def wait_kv(n):
        to = (W.at[0, pl.ds(0, HALF), pl.ds(0, 256)], W.at[0, pl.ds(HALF, HALF), pl.ds(0, 256)], W.at[0, :, pl.ds(256, 256)], W.at[1])[n]
        pltpu.make_async_copy(to, to, kvsem.at[n]).wait()

    def slot_sem(s):
        return wsem.at[s - 2] if s >= 2 else kvsem.at[s]

    def load_q(s):
        at = pl.multiple_of(2048 * c + N * s, N)
        pltpu.make_async_copy(wq.at[:, pl.ds(at, N)], W.at[2 + s], slot_sem(2 + s)).start(priority=1)

    def load_o(k, slot):
        side = c if k % 2 == 0 else 1 - c
        row = pl.multiple_of(2048 * side + 1024 * (k // 2), 1024)
        for n in range(NB):
            at = pl.multiple_of(COLS * c + N * n, N)
            to = W.at[slot, pl.ds(1024 * n, 1024), :]
            pltpu.make_async_copy(wo.at[pl.ds(row, 1024), pl.ds(at, N)], to, slot_sem(slot)).start(priority=1)

    def arrive(to, sem):
        pltpu.make_async_copy(to, to, sem).wait()

    def wait_slot(s):
        pltpu.make_async_copy(W.at[s], W.at[s], slot_sem(s)).wait()

    own_rows = pl.ds(pl.multiple_of(c * OWN, OWN), OWN)
    their_rows = pl.ds(pl.multiple_of((1 - c) * OWN, OWN), OWN)
    own_columns = pl.ds(pl.multiple_of(COLS * c, N), COLS)
    their_columns = pl.ds(pl.multiple_of(COLS * (1 - c), N), COLS)

    def rows_of(half, i):
        return pl.ds(pl.multiple_of(half * OWN + i * PIECE, PIECE), PIECE)

    x_in = [pltpu.make_async_copy(x_hbm.at[i * PIECE : (i + 1) * PIECE], xr.at[rows_of(c, i)], xsem.at[i]) for i in range(PIECES)]
    gain_in = pltpu.make_async_copy(gain_hbm, gain, tsem.at[0])
    gain_in.start()
    for piece in x_in:
        piece.start()
    places = pl.ds(pl.multiple_of(chip * TOK, TOK), TOK)
    turns_in = pltpu.make_async_copy(turns_hbm.at[places], cos, tsem.at[1])
    turns_in.start()
    for h in range(4):
        load_kv(h)
    for s in range(4):
        load_q(s)
    load_o(0, 6)
    load_o(1, 7)

    barrier = pltpu.get_barrier_semaphore()
    for peer in (partner, there(chip + 1 - 2 * (chip % 2)), there((chip + 2) % 4)):
        pl.semaphore_signal(barrier, inc=1, device_id=peer, device_id_type=mesh_id)
    pl.semaphore_wait(barrier, 3)

    gain_in.wait()
    gain8[...] = jnp.broadcast_to(gain[...].astype(F32)[None, :], (8, D))

    def norm_copy(i):
        part = a.at[rows_of(c, i), pl.ds(0, HALF)] if i < PIECES else a.at[own_rows, pl.ds(HALF, HALF)]
        return pltpu.make_async_remote_copy(part, part, nsend, nrecv.at[i // PIECES], partner, mesh_id)

    for i in range(PIECES):
        x_in[i].wait()
        first = c * OWN + i * PIECE
        groups = [pl.ds(pl.multiple_of(first + n * 16, 16), 16) for n in range(PIECE // 16)]
        scales = []
        for rows in groups:
            total = jnp.zeros((16, HEAD), F32)
            for at in range(0, D, HEAD):
                wide = xr[rows, at : at + HEAD].astype(F32)
                total += wide * wide
            scales.append(lax.rsqrt(jnp.sum(total, -1, keepdims=True) * (1 / D) + 1e-6))
        for at in range(0, D, HEAD):
            g = jnp.concatenate([gain8[:, at : at + HEAD]] * 2, 0)
            for rows, scale in zip(groups, scales):
                a[rows, at : at + HEAD] = (xr[rows, at : at + HEAD].astype(F32) * scale * g).astype(BF16)
        norm_copy(i).start()
    norm_copy(PIECES).start()

    turns_in.wait()
    both = cos[...]
    other = pltpu.roll(both, 64, 1)
    low = lax.broadcasted_iota(jnp.int32, (TOK, HEAD), 1) < HEAD // 2
    cos[...] = jnp.where(low, both, other)
    sin[...] = jnp.where(low, -other, both)

    def turn(t, rows):
        t = t.astype(BF16).astype(F32)
        return (t * cos[rows, :] + pltpu.roll(t, 64, 1) * sin[rows, :]).astype(BF16)

    def unit_copy(j, h, half, sem, chip_to, count):
        unit = kv.at[j, h, half]
        return pltpu.make_async_remote_copy(unit, unit, sem, krecv.at[count], there(chip_to), mesh_id)

    def arrived(units, count):
        pltpu.make_async_copy(units, units, krecv.at[count]).wait()

    def make_kv(rows, halves, heads, gates):
        lo = (heads[0] % 2) * 2 * HEAD
        columns = slice(lo, lo + len(heads) * 2 * HEAD)
        gates[0]()
        r = _dot(a[rows, :HALF], W[heads[0] // 2, :HALF, columns])
        gates[1]()
        r += _dot(a[rows, HALF:], W[heads[0] // 2, HALF:, columns])
        for i, h in enumerate(heads):
            keys = turn(r[:, i * 256 : i * 256 + HEAD], rows)
            values = r[:, i * 256 + HEAD : (i + 1) * 256].astype(BF16)
            for n, half in enumerate(halves):
                kv[chip, h, half, :, :HEAD] = keys[n * OWN : (n + 1) * OWN]
                kv[chip, h, half, :, HEAD:] = values[n * OWN : (n + 1) * OWN]

    def send(own, h, chips=(0, 1, 2)):
        half = c if own else 1 - c
        if 0 in chips:
            @pl.when(chip == 0)
            def _():
                for n in range(2):
                    unit_copy(chip, h, half, ksend.at[n], n + 1, jnp.where(half == n, h, 4 + h // 2)).start()

        if 1 in chips:
            @pl.when((chip == 1) | (chip == 2))
            def _():
                count = jnp.where(chip == 2, 2 + h // 2, 4 + h if own else min(8 + h, 10))
                unit_copy(chip, h, half, ksend.at[0], 3, count).start()

    def pass_on(own, h, by=3):
        half = c if own else 1 - c

        @pl.when(chip == by)
        def _():
            arrived(kv.at[1, h, half], h - 2 if by == 0 else 4 + h if own else 8 + h)
            unit_copy(1, h, half, rsend, 2, 6 + h // 2).start()

    def relay(h):
        for p in (1, 2):
            @pl.when(chip == p)
            def _():
                arrived(kv.at[0, h, p - 1], h)
                unit_copy(0, h, p - 1, rsend, 3, h // 2).start()

    def gate(*waits):
        def run():
            for wait in waits:
                wait()
        return run

    make_kv(own_rows, (c,), (0,), (gate(functools.partial(wait_kv, 0)), gate(functools.partial(wait_kv, 1))))
    send(True, 0)
    make_kv(own_rows, (c,), (1,), (gate(functools.partial(wait_kv, 2)), gate()))
    send(True, 1)
    def theirs_here(n):
        part = a.at[their_rows, pl.ds(n * HALF, HALF)]
        pltpu.make_async_copy(part, part, nrecv.at[n]).wait()

    halves = gate(functools.partial(theirs_here, 0)), gate(functools.partial(theirs_here, 1))
    make_kv(their_rows, (1 - c,), (0, 1), halves)
    send(False, 0)
    send(False, 1)
    make_kv(pl.ds(0, TOK), (0, 1), (2, 3), (gate(functools.partial(wait_kv, 3)), gate()))
    for h in (2, 3):
        send(True, h)
    for h in (2, 3):
        send(False, h, (0,))

        @pl.when(chip == 1)
        def _():
            unit_copy(chip, h, 1 - c, ksend.at[1], 0, h - 2).start()

    load_o(2, 0)
    load_o(3, 1)
    x_out = pltpu.make_async_remote_copy(x_hbm.at[:, their_columns], xr.at[own_rows, their_columns], xsend, xrecv, partner, mesh_id)
    x_out.start()
    pass_on(True, 0)

    def put_q(s, r):
        for g in range(4):
            q[s, g * TOK : (g + 1) * TOK, :] = turn(r[:, g * HEAD : (g + 1) * HEAD], pl.ds(0, TOK))

    for s in range(4):
        wait_slot(2 + s)
        r = _dot(a[...], W[2 + s])
        if s:
            put_q(s - 1, before)
        before = r
        if s == 0:
            pass_on(True, 1)
        if s == 1:
            pass_on(False, 0)
            relay(0)
        if s == 2:
            pass_on(False, 1)
            relay(1)
            send(False, 2, (1,))
            send(False, 3, (1,))

    def attend(heads, js, first=False, beside=()):
        mask = None
        if first:
            mask = lax.broadcasted_iota(jnp.int32, (TOK, TOK), 0) <= lax.broadcasted_iota(jnp.int32, (TOK, TOK), 1)
        units = [(h, slice(g * TOK, (g + 1) * TOK)) for h in heads for g in range(4)]
        chunks, scores, weights, keeps = {}, {}, {}, {}

        def score(n):
            h, at = units[n]
            if h not in chunks:
                chunks[h] = []
                for j in js:
                    values = jnp.concatenate([kv[j, h, t, :, HEAD:] for t in range(2)], 0)
                    chunks[h].append((jnp.concatenate([kv[j, h, t, :, :HEAD] for t in range(2)], 0),
                                      jnp.concatenate([values.T, jnp.ones((8, TOK), BF16)], 0)))
            scores[n] = [_dot(keys, q[h, at, :], 1, 1) for keys, _ in chunks[h]]

        def weigh(n):
            h, at = units[n]
            some = scores.pop(n)
            if first:
                some = [jnp.where(mask, s, HIDDEN) for s in some]
            tops = [s.max(axis=0, keepdims=True) for s in some]
            top = functools.reduce(jnp.maximum, tops)
            if not first:
                old = top_s[h, :, at]
                top = jnp.maximum(old, top)
                keeps[n] = jnp.exp2((old - top) * E)
            top_s[h, :, at] = top
            weights[n] = [jnp.exp2((s - top) * E).astype(BF16) for s in some]

        def add(n):
            h, at = units[n]
            parts = [_dot(vt, p) for p, (_, vt) in zip(weights.pop(n), chunks[h])]
            total = functools.reduce(jnp.add, parts)
            acc[h, :, at] = total if first else acc[h, :, at] * keeps.pop(n) + total

        ahead = 4 if len(js) == 1 else 2
        steps = len(units) + ahead + 1
        for n in range(steps):
            if n < len(units):
                score(n)
            for piece in beside[len(beside) * n // steps : len(beside) * (n + 1) // steps]:
                piece()
            if 0 <= n - ahead < len(units):
                weigh(n - ahead)
            if 0 <= n - ahead - 1:
                add(n - ahead - 1)

    put_q(3, before)
    attend(range(4), [chip], True)
    pass_on(True, 2)
    pass_on(True, 3)
    pass_on(False, 2, 0)
    pass_on(False, 3, 0)

    def early(pair, beside=()):
        heads = (2 * pair, 2 * pair + 1)

        @pl.when(chip == 3)
        def _():
            if pair == 1:
                arrived(kv.at[1, pl.ds(2, 2), 1 - c], 10)
            arrived(kv.at[2, pl.ds(2 * pair, 2)], 2 + pair)
            attend(heads, [1, 2], beside=beside)

    def swap(pair, rows, sem):
        return pltpu.make_async_remote_copy(mine.at[pair, rows], theirs.at[pair, rows], asend, arecv.at[sem], partner, mesh_id)

    def late(pair):
        heads = (2 * pair, 2 * pair + 1)

        def chunk(j, _):
            @pl.when(chip == 1)
            def _():
                arrived(kv.at[0, pl.ds(2 * pair, 2), 1], 4 + pair)

            @pl.when((chip == 2) & (j == 0))
            def _():
                arrived(kv.at[0, pl.ds(2 * pair, 2), 0], 4 + pair)

            @pl.when((chip == 2) & (j == 1))
            def _():
                arrived(kv.at[1, pl.ds(2 * pair, 2)], 6 + pair)

            @pl.when(chip == 3)
            def _():
                arrived(kv.at[0, pl.ds(2 * pair, 2)], pair)

            attend(heads, [j])

        lax.fori_loop(0, jnp.where(chip == 2, 2, jnp.minimum(chip, 1)), chunk, None)

        def finish(first, rows):
            for i, h in enumerate(heads):
                for g in range(4):
                    at = pl.ds(pl.multiple_of(g * TOK + first, OWN), rows.size)
                    out = acc[h, :HEAD, at] * (1 / acc[h, HEAD : HEAD + 1, at])
                    mine[pair, rows, (4 * i + g) * HEAD : (4 * i + g + 1) * HEAD] = out.astype(BF16).T

        if pair == 0:
            finish(c * OWN, own_rows)
            swap(0, own_rows, 0).start()
            finish((1 - c) * OWN, their_rows)
            swap(0, their_rows, 0).start()
        else:
            finish(c * OWN, own_rows)
            swap(1, own_rows, 1).start()
            finish((1 - c) * OWN, their_rows)
            swap(1, their_rows, 2).start()

    def blocks(slot, n):
        return W[slot, 1024 * n : 1024 * (n + 1), :]

    early(0)
    relay(2)
    late(0)
    relay(3)
    wait_slot(6)
    for n in range(NB):
        y[n] = _dot(mine[0], blocks(6, n))
    arrive(theirs.at[0], arecv.at[0])
    wait_slot(7)

    def second_product(n, lo):
        y[n, :, lo : lo + TOK] += _dot(theirs[0], blocks(7, n)[:, lo : lo + TOK])

    pieces = [functools.partial(second_product, n, lo) for n in range(NB) for lo in range(0, N, TOK)]
    early(1, pieces)

    @pl.when(chip < 3)
    def _():
        for piece in pieces:
            piece()

    late(1)
    wait_slot(0)

    def third(n, rows):
        return _dot(mine[1, rows], blocks(0, n))

    for n in range(NB):
        y[n, their_rows] += third(n, their_rows)
    for n in range(3):
        y[n, own_rows] += third(n, own_rows)
    wait_slot(1)
    x_out.wait_recv()
    arrive(theirs.at[1, their_rows], arecv.at[1])

    def out_copy(n):
        at = pl.ds(pl.multiple_of(COLS * c + N * n, N), N)
        return pltpu.make_async_remote_copy(yo.at[n], y_out.at[:, at], ysend, yrecv, partner, mesh_id)

    def result(n, rows, more=False):
        at = pl.ds(pl.multiple_of(COLS * c + N * n, N), N)
        r = _dot(theirs[1, rows], blocks(1, n))
        r = y[n, rows] + (third(n, rows) + r if more else r)
        return (xr[rows, at].astype(F32) + r).astype(BF16), at

    for group in ((0, 1), (2, 3), (4,)):
        for n in group:
            yo[n], _ = result(n, their_rows)
        for n in group:
            out_copy(n).start()
    arrive(theirs.at[1, own_rows], arecv.at[2])
    for n in range(NB):
        part, at = result(n, own_rows, n >= 3)
        y_out[:, at] = part

    x_out.wait_send()
    arrive(a.at[own_rows], nsend)
    arrive(mine, asend)

    @pl.when(chip != 3)
    def _():
        arrive(kv.at[0], ksend.at[0])

    @pl.when(chip == 0)
    def _():
        arrive(kv.at[0], ksend.at[1])
        arrive(kv.at[0, pl.ds(0, 2), 0], rsend)

    @pl.when(chip == 1)
    def _():
        arrive(kv.at[0, pl.ds(0, 2), 0], ksend.at[1])

    @pl.when((chip == 1) | (chip == 2))
    def _():
        arrive(kv.at[0, pl.ds(0, 4), 0], rsend)

    @pl.when(chip == 3)
    def _():
        arrive(kv.at[0, pl.ds(0, 3)], rsend)

    arrive(yo, ysend)
    arrive(y_out.at[:, their_columns], yrecv)


def solution(mesh):
    turns = tables(4 * TOK)

    def step(x, gain, wq, wk, wv, wo):
        anywhere = pl.BlockSpec(memory_space=pl.ANY)
        dma = pltpu.SemaphoreType.DMA
        return pl.pallas_call(
            kernel,
            out_shape=pltpu.VMEM((OWN, D), BF16),
            in_specs=[anywhere] * 7,
            out_specs=pl.BlockSpec(memory_space=pltpu.VMEM),
            scratch_shapes=[
                pltpu.VMEM((SLOTS, D, N), BF16),
                pltpu.VMEM((TOK, D), BF16),
                pltpu.VMEM((TOK, D), BF16),
                pltpu.VMEM((D,), BF16),
                pltpu.VMEM((8, D), F32),
                pltpu.VMEM((TOK, HEAD), F32),
                pltpu.VMEM((TOK, HEAD), F32),
                pltpu.VMEM((4, 4 * TOK, HEAD), BF16),
                pltpu.VMEM((4, 4, 2, OWN, 2 * HEAD), BF16),
                pltpu.VMEM((4, HEAD + 8, 4 * TOK), F32),
                pltpu.VMEM((4, 1, 4 * TOK), F32),
                pltpu.VMEM((2, TOK, 1024), BF16),
                pltpu.VMEM((2, TOK, 1024), BF16),
                pltpu.VMEM((NB, TOK, N), F32),
                pltpu.VMEM((NB, OWN, N), BF16),
                dma((SLOTS - 2,)), dma((4,)), dma((PIECES,)), dma((2,)), dma, dma, dma, dma((2,)),
                dma((2,)), dma((11,)), dma, dma, dma((3,)), dma, dma,
            ],
            compiler_params=pltpu.CompilerParams(collective_id=0, has_side_effects=True, vmem_limit_bytes=62 * 2**20),
        )(x, gain, wq, wk, wv, wo, jnp.asarray(turns))

    tokens, whole = P(("dp", "sp"), None), P(None, None)
    return jax.shard_map(step, mesh=mesh, in_specs=(tokens, P(None), whole, whole, whole, whole), out_specs=tokens, check_vma=False)
```

```python
import functools

import jax
import jax.numpy as jnp
import numpy as np
from jax import lax
from jax.experimental import pallas as pl
from jax.experimental.pallas import tpu as pltpu
from jax.sharding import PartitionSpec as P

HEAD = 128
THETA = 10000
LOG2E = 1.4426950408889634
HIDDEN = -2e30
E = HEAD**-0.5 * LOG2E
F32, BF16 = jnp.float32, jnp.bfloat16

OWN = 128
TOK = 256
D = 5120
N = 512
COLS = D // 2
HALF = D // 2
NB = COLS // N
SLOTS = 8
PIECE = 64
PIECES = OWN // PIECE


def tables(rows):
    half = HEAD // 2
    power = np.float32(THETA) ** (-np.arange(half, dtype=np.float32) / np.float32(half))
    angle = np.arange(rows, dtype=np.float32)[:, None] * power.astype(np.float32)
    cos, sin = np.cos(angle.astype(np.float32)), np.sin(angle.astype(np.float32))
    return np.concatenate([cos, sin], 1).astype(np.float32)


def _dot(a, b, ca=1, cb=0):
    return lax.dot_general(a, b, (((ca,), (cb,)), ((), ())), preferred_element_type=F32)


def kernel(x_hbm, gain_hbm, wq, wk, wv, wo, turns_hbm, y_out,
           W, xr, a, gain, gain8, cos, sin, q, kv, acc, top_s, mine, theirs, y, yo,
           wsem, kvsem, xsem, tsem, xsend, xrecv, nsend, nrecv, ksend, krecv, rsend, asend, arecv, ysend, yrecv):
    me = lax.axis_index("sp")
    chip, c = me // 2, me % 2
    partner = {"sp": chip * 2 + (1 - c)}
    mesh_id = pl.DeviceIdType.MESH

    def there(chip_to):
        return {"sp": chip_to * 2 + c}

    def load_kv(h):
        at = pl.multiple_of((4 * c + h) * HEAD, HEAD)
        for part in range(2):
            rows = pl.ds(part * HALF, HALF)
            for n, w in enumerate((wk, wv)):
                to = W.at[h // 2, rows, pl.ds((h % 2) * 2 * HEAD + n * HEAD, HEAD)]
                sem = kvsem.at[part if h == 0 else min(h, 2) + 1]
                pltpu.make_async_copy(w.at[rows, pl.ds(at, HEAD)], to, sem).start(priority=1)

    def wait_kv(n):
        to = (W.at[0, pl.ds(0, HALF), pl.ds(0, 256)], W.at[0, pl.ds(HALF, HALF), pl.ds(0, 256)], W.at[0, :, pl.ds(256, 256)], W.at[1])[n]
        pltpu.make_async_copy(to, to, kvsem.at[n]).wait()

    def slot_sem(s):
        return wsem.at[s - 2] if s >= 2 else kvsem.at[s]

    def load_q(s):
        at = pl.multiple_of(2048 * c + N * s, N)
        pltpu.make_async_copy(wq.at[:, pl.ds(at, N)], W.at[2 + s], slot_sem(2 + s)).start(priority=1)

    def load_o(k, slot):
        side = c if k % 2 == 0 else 1 - c
        row = pl.multiple_of(2048 * side + 1024 * (k // 2), 1024)
        for n in range(NB):
            at = pl.multiple_of(COLS * c + N * n, N)
            to = W.at[slot, pl.ds(1024 * n, 1024), :]
            pltpu.make_async_copy(wo.at[pl.ds(row, 1024), pl.ds(at, N)], to, slot_sem(slot)).start(priority=1)

    def arrive(to, sem):
        pltpu.make_async_copy(to, to, sem).wait()

    def wait_slot(s):
        pltpu.make_async_copy(W.at[s], W.at[s], slot_sem(s)).wait()

    own_rows = pl.ds(pl.multiple_of(c * OWN, OWN), OWN)
    their_rows = pl.ds(pl.multiple_of((1 - c) * OWN, OWN), OWN)
    own_columns = pl.ds(pl.multiple_of(COLS * c, N), COLS)
    their_columns = pl.ds(pl.multiple_of(COLS * (1 - c), N), COLS)

    def rows_of(half, i):
        return pl.ds(pl.multiple_of(half * OWN + i * PIECE, PIECE), PIECE)

    x_in = [pltpu.make_async_copy(x_hbm.at[i * PIECE : (i + 1) * PIECE], xr.at[rows_of(c, i)], xsem.at[i]) for i in range(PIECES)]
    gain_in = pltpu.make_async_copy(gain_hbm, gain, tsem.at[0])
    gain_in.start()
    for piece in x_in:
        piece.start()
    places = pl.ds(pl.multiple_of(chip * TOK, TOK), TOK)
    turns_in = pltpu.make_async_copy(turns_hbm.at[places], cos, tsem.at[1])
    turns_in.start()
    for h in range(4):
        load_kv(h)
    for s in range(4):
        load_q(s)
    load_o(0, 6)
    load_o(1, 7)

    barrier = pltpu.get_barrier_semaphore()
    for peer in (partner, there(chip + 1 - 2 * (chip % 2)), there((chip + 2) % 4)):
        pl.semaphore_signal(barrier, inc=1, device_id=peer, device_id_type=mesh_id)
    pl.semaphore_wait(barrier, 3)

    gain_in.wait()
    gain8[...] = jnp.broadcast_to(gain[...].astype(F32)[None, :], (8, D))

    def norm_copy(i):
        part = a.at[rows_of(c, i), pl.ds(0, HALF)] if i < PIECES else a.at[own_rows, pl.ds(HALF, HALF)]
        return pltpu.make_async_remote_copy(part, part, nsend, nrecv.at[i // PIECES], partner, mesh_id)

    for i in range(PIECES):
        x_in[i].wait()
        first = c * OWN + i * PIECE
        groups = [pl.ds(pl.multiple_of(first + n * 16, 16), 16) for n in range(PIECE // 16)]
        scales = []
        for rows in groups:
            total = jnp.zeros((16, HEAD), F32)
            for at in range(0, D, HEAD):
                wide = xr[rows, at : at + HEAD].astype(F32)
                total += wide * wide
            scales.append(lax.rsqrt(jnp.sum(total, -1, keepdims=True) * (1 / D) + 1e-6))
        for at in range(0, D, HEAD):
            g = jnp.concatenate([gain8[:, at : at + HEAD]] * 2, 0)
            for rows, scale in zip(groups, scales):
                a[rows, at : at + HEAD] = (xr[rows, at : at + HEAD].astype(F32) * scale * g).astype(BF16)
        norm_copy(i).start()
    norm_copy(PIECES).start()

    turns_in.wait()
    both = cos[...]
    other = pltpu.roll(both, 64, 1)
    low = lax.broadcasted_iota(jnp.int32, (TOK, HEAD), 1) < HEAD // 2
    cos[...] = jnp.where(low, both, other)
    sin[...] = jnp.where(low, -other, both)

    def turn(t, rows):
        t = t.astype(BF16).astype(F32)
        return (t * cos[rows, :] + pltpu.roll(t, 64, 1) * sin[rows, :]).astype(BF16)

    def unit_copy(j, h, half, sem, chip_to, count):
        unit = kv.at[j, h, half]
        return pltpu.make_async_remote_copy(unit, unit, sem, krecv.at[count], there(chip_to), mesh_id)

    def arrived(units, count):
        pltpu.make_async_copy(units, units, krecv.at[count]).wait()

    def make_kv(rows, halves, heads, gates):
        lo = (heads[0] % 2) * 2 * HEAD
        columns = slice(lo, lo + len(heads) * 2 * HEAD)
        gates[0]()
        r = _dot(a[rows, :HALF], W[heads[0] // 2, :HALF, columns])
        gates[1]()
        r += _dot(a[rows, HALF:], W[heads[0] // 2, HALF:, columns])
        for i, h in enumerate(heads):
            keys = turn(r[:, i * 256 : i * 256 + HEAD], rows)
            values = r[:, i * 256 + HEAD : (i + 1) * 256].astype(BF16)
            for n, half in enumerate(halves):
                kv[chip, h, half, :, :HEAD] = keys[n * OWN : (n + 1) * OWN]
                kv[chip, h, half, :, HEAD:] = values[n * OWN : (n + 1) * OWN]

    def send(own, h, chips=(0, 1, 2)):
        half = c if own else 1 - c
        if 0 in chips:
            @pl.when(chip == 0)
            def _():
                for n in range(2):
                    unit_copy(chip, h, half, ksend.at[n], n + 1, jnp.where(half == n, h, 4 + h // 2)).start()

        if 1 in chips:
            @pl.when((chip == 1) | (chip == 2))
            def _():
                count = jnp.where(chip == 2, 2 + h // 2, 4 + h if own else min(8 + h, 10))
                unit_copy(chip, h, half, ksend.at[0], 3, count).start()

    def pass_on(own, h, by=3):
        half = c if own else 1 - c

        @pl.when(chip == by)
        def _():
            arrived(kv.at[1, h, half], h - 2 if by == 0 else 4 + h if own else 8 + h)
            unit_copy(1, h, half, rsend, 2, 6 + h // 2).start()

    def relay(h):
        for p in (1, 2):
            @pl.when(chip == p)
            def _():
                arrived(kv.at[0, h, p - 1], h)
                unit_copy(0, h, p - 1, rsend, 3, h // 2).start()

    def gate(*waits):
        def run():
            for wait in waits:
                wait()
        return run

    make_kv(own_rows, (c,), (0,), (gate(functools.partial(wait_kv, 0)), gate(functools.partial(wait_kv, 1))))
    send(True, 0)
    make_kv(own_rows, (c,), (1,), (gate(functools.partial(wait_kv, 2)), gate()))
    send(True, 1)
    def theirs_here(n):
        part = a.at[their_rows, pl.ds(n * HALF, HALF)]
        pltpu.make_async_copy(part, part, nrecv.at[n]).wait()

    halves = gate(functools.partial(theirs_here, 0)), gate(functools.partial(theirs_here, 1))
    make_kv(their_rows, (1 - c,), (0, 1), halves)
    send(False, 0)
    send(False, 1)
    make_kv(pl.ds(0, TOK), (0, 1), (2, 3), (gate(functools.partial(wait_kv, 3)), gate()))
    for h in (2, 3):
        send(True, h)
    for h in (2, 3):
        send(False, h, (0,))

        @pl.when(chip == 1)
        def _():
            unit_copy(chip, h, 1 - c, ksend.at[1], 0, h - 2).start()

    load_o(2, 0)
    load_o(3, 1)
    x_out = pltpu.make_async_remote_copy(x_hbm.at[:, their_columns], xr.at[own_rows, their_columns], xsend, xrecv, partner, mesh_id)
    x_out.start()
    pass_on(True, 0)

    def put_q(s, r):
        for g in range(4):
            q[s, g * TOK : (g + 1) * TOK, :] = turn(r[:, g * HEAD : (g + 1) * HEAD], pl.ds(0, TOK))

    for s in range(4):
        wait_slot(2 + s)
        r = _dot(a[...], W[2 + s])
        if s:
            put_q(s - 1, before)
        before = r
        if s == 0:
            pass_on(True, 1)
        if s == 1:
            pass_on(False, 0)
            relay(0)
        if s == 2:
            pass_on(False, 1)
            relay(1)
            send(False, 2, (1,))
            send(False, 3, (1,))

    def attend(heads, js, first=False, beside=()):
        mask = None
        if first:
            mask = lax.broadcasted_iota(jnp.int32, (TOK, TOK), 0) <= lax.broadcasted_iota(jnp.int32, (TOK, TOK), 1)
        units = [(h, slice(g * TOK, (g + 1) * TOK)) for h in heads for g in range(4)]
        chunks, scores, weights, keeps = {}, {}, {}, {}

        def score(n):
            h, at = units[n]
            if h not in chunks:
                chunks[h] = []
                for j in js:
                    values = jnp.concatenate([kv[j, h, t, :, HEAD:] for t in range(2)], 0)
                    chunks[h].append((jnp.concatenate([kv[j, h, t, :, :HEAD] for t in range(2)], 0),
                                      jnp.concatenate([values.T, jnp.ones((8, TOK), BF16)], 0)))
            scores[n] = [_dot(keys, q[h, at, :], 1, 1) for keys, _ in chunks[h]]

        def weigh(n):
            h, at = units[n]
            some = scores.pop(n)
            if first:
                some = [jnp.where(mask, s, HIDDEN) for s in some]
            tops = [s.max(axis=0, keepdims=True) for s in some]
            top = functools.reduce(jnp.maximum, tops)
            if not first:
                old = top_s[h, :, at]
                top = jnp.maximum(old, top)
                keeps[n] = jnp.exp2((old - top) * E)
            top_s[h, :, at] = top
            weights[n] = [jnp.exp2((s - top) * E).astype(BF16) for s in some]

        def add(n):
            h, at = units[n]
            parts = [_dot(vt, p) for p, (_, vt) in zip(weights.pop(n), chunks[h])]
            total = functools.reduce(jnp.add, parts)
            acc[h, :, at] = total if first else acc[h, :, at] * keeps.pop(n) + total

        ahead = 4 if len(js) == 1 else 2
        steps = len(units) + ahead + 1
        for n in range(steps):
            if n < len(units):
                score(n)
            for piece in beside[len(beside) * n // steps : len(beside) * (n + 1) // steps]:
                piece()
            if 0 <= n - ahead < len(units):
                weigh(n - ahead)
            if 0 <= n - ahead - 1:
                add(n - ahead - 1)

    put_q(3, before)
    attend(range(4), [chip], True)
    pass_on(True, 2)
    pass_on(True, 3)
    pass_on(False, 2, 0)
    pass_on(False, 3, 0)

    def early(pair, beside=()):
        heads = (2 * pair, 2 * pair + 1)

        @pl.when(chip == 3)
        def _():
            if pair == 1:
                arrived(kv.at[1, pl.ds(2, 2), 1 - c], 10)
            arrived(kv.at[2, pl.ds(2 * pair, 2)], 2 + pair)
            attend(heads, [1, 2], beside=beside)

    def swap(pair, rows, sem):
        return pltpu.make_async_remote_copy(mine.at[pair, rows], theirs.at[pair, rows], asend, arecv.at[sem], partner, mesh_id)

    def late(pair):
        heads = (2 * pair, 2 * pair + 1)

        def chunk(j, _):
            @pl.when(chip == 1)
            def _():
                arrived(kv.at[0, pl.ds(2 * pair, 2), 1], 4 + pair)

            @pl.when((chip == 2) & (j == 0))
            def _():
                arrived(kv.at[0, pl.ds(2 * pair, 2), 0], 4 + pair)

            @pl.when((chip == 2) & (j == 1))
            def _():
                arrived(kv.at[1, pl.ds(2 * pair, 2)], 6 + pair)

            @pl.when(chip == 3)
            def _():
                arrived(kv.at[0, pl.ds(2 * pair, 2)], pair)

            attend(heads, [j])

        lax.fori_loop(0, jnp.where(chip == 2, 2, jnp.minimum(chip, 1)), chunk, None)

        def finish(first, rows):
            for i, h in enumerate(heads):
                for g in range(4):
                    at = pl.ds(pl.multiple_of(g * TOK + first, OWN), rows.size)
                    out = acc[h, :HEAD, at] * (1 / acc[h, HEAD : HEAD + 1, at])
                    mine[pair, rows, (4 * i + g) * HEAD : (4 * i + g + 1) * HEAD] = out.astype(BF16).T

        if pair == 0:
            finish(c * OWN, own_rows)
            swap(0, own_rows, 0).start()
            finish((1 - c) * OWN, their_rows)
            swap(0, their_rows, 0).start()
        else:
            finish(c * OWN, own_rows)
            swap(1, own_rows, 1).start()
            finish((1 - c) * OWN, their_rows)
            swap(1, their_rows, 2).start()

    def blocks(slot, n):
        return W[slot, 1024 * n : 1024 * (n + 1), :]

    early(0)
    relay(2)
    late(0)
    relay(3)
    wait_slot(6)
    for n in range(NB):
        y[n] = _dot(mine[0], blocks(6, n))
    arrive(theirs.at[0], arecv.at[0])
    wait_slot(7)

    def second_product(n, lo):
        y[n, :, lo : lo + TOK] += _dot(theirs[0], blocks(7, n)[:, lo : lo + TOK])

    pieces = [functools.partial(second_product, n, lo) for n in range(NB) for lo in range(0, N, TOK)]
    early(1, pieces)

    @pl.when(chip < 3)
    def _():
        for piece in pieces:
            piece()

    late(1)
    wait_slot(0)

    def third(n, rows):
        return _dot(mine[1, rows], blocks(0, n))

    for n in range(NB):
        y[n, their_rows] += third(n, their_rows)
    for n in range(2):
        y[n, own_rows] += third(n, own_rows)
    wait_slot(1)
    x_out.wait_recv()
    arrive(theirs.at[1, their_rows], arecv.at[1])

    def out_copy(n):
        at = pl.ds(pl.multiple_of(COLS * c + N * n, N), N)
        return pltpu.make_async_remote_copy(yo.at[n], y_out.at[:, at], ysend, yrecv, partner, mesh_id)

    def result(n, rows, more=False):
        at = pl.ds(pl.multiple_of(COLS * c + N * n, N), N)
        r = _dot(theirs[1, rows], blocks(1, n))
        r = y[n, rows] + (third(n, rows) + r if more else r)
        return (xr[rows, at].astype(F32) + r).astype(BF16), at

    for group in ((0, 1), (2, 3), (4,)):
        for n in group:
            yo[n], _ = result(n, their_rows)
        for n in group:
            out_copy(n).start()
    arrive(theirs.at[1, own_rows], arecv.at[2])
    for n in range(NB):
        part, at = result(n, own_rows, n >= 2)
        y_out[:, at] = part

    x_out.wait_send()
    arrive(a.at[own_rows], nsend)
    arrive(mine, asend)

    @pl.when(chip != 3)
    def _():
        arrive(kv.at[0], ksend.at[0])

    @pl.when(chip == 0)
    def _():
        arrive(kv.at[0], ksend.at[1])
        arrive(kv.at[0, pl.ds(0, 2), 0], rsend)

    @pl.when(chip == 1)
    def _():
        arrive(kv.at[0, pl.ds(0, 2), 0], ksend.at[1])

    @pl.when((chip == 1) | (chip == 2))
    def _():
        arrive(kv.at[0, pl.ds(0, 4), 0], rsend)

    @pl.when(chip == 3)
    def _():
        arrive(kv.at[0, pl.ds(0, 3)], rsend)

    arrive(yo, ysend)
    arrive(y_out.at[:, their_columns], yrecv)


def solution(mesh):
    turns = tables(4 * TOK)

    def step(x, gain, wq, wk, wv, wo):
        anywhere = pl.BlockSpec(memory_space=pl.ANY)
        dma = pltpu.SemaphoreType.DMA
        return pl.pallas_call(
            kernel,
            out_shape=pltpu.VMEM((OWN, D), BF16),
            in_specs=[anywhere] * 7,
            out_specs=pl.BlockSpec(memory_space=pltpu.VMEM),
            scratch_shapes=[
                pltpu.VMEM((SLOTS, D, N), BF16),
                pltpu.VMEM((TOK, D), BF16),
                pltpu.VMEM((TOK, D), BF16),
                pltpu.VMEM((D,), BF16),
                pltpu.VMEM((8, D), F32),
                pltpu.VMEM((TOK, HEAD), F32),
                pltpu.VMEM((TOK, HEAD), F32),
                pltpu.VMEM((4, 4 * TOK, HEAD), BF16),
                pltpu.VMEM((4, 4, 2, OWN, 2 * HEAD), BF16),
                pltpu.VMEM((4, HEAD + 8, 4 * TOK), F32),
                pltpu.VMEM((4, 1, 4 * TOK), F32),
                pltpu.VMEM((2, TOK, 1024), BF16),
                pltpu.VMEM((2, TOK, 1024), BF16),
                pltpu.VMEM((NB, TOK, N), F32),
                pltpu.VMEM((NB, OWN, N), BF16),
                dma((SLOTS - 2,)), dma((4,)), dma((PIECES,)), dma((2,)), dma, dma, dma, dma((2,)),
                dma((2,)), dma((11,)), dma, dma, dma((3,)), dma, dma,
            ],
            compiler_params=pltpu.CompilerParams(collective_id=0, has_side_effects=True, vmem_limit_bytes=62 * 2**20),
        )(x, gain, wq, wk, wv, wo, jnp.asarray(turns))

    tokens, whole = P(("dp", "sp"), None), P(None, None)
    return jax.shard_map(step, mesh=mesh, in_specs=(tokens, P(None), whole, whole, whole, whole), out_specs=tokens, check_vma=False)
```
